8 devices in a mesh: dp: 1 (over z), ep: 8 (over y, x, core).
Axes of the slice: x: 2, y: 2, z: 1, core: 2. Of those that a mesh axis runs over, the one named last changes fastest.
Arguments:
- h0: bfloat16 [8, 256, 2048], P(('dp', 'ep'))
- idx: int32 [8, 256, 8], P(('dp', 'ep'))
- slot: int32 [8, 256, 8], P(('dp', 'ep'))
- norm_attn: bfloat16 [2048], replicated
- wq: bfloat16 [2048, 4096], replicated
- wk: bfloat16 [2048, 512], replicated
- wv: bfloat16 [2048, 512], replicated
- wo: bfloat16 [4096, 2048], replicated
- norm_ffn: bfloat16 [2048], replicated
- w1: bfloat16 [2048, 6144], replicated
- w3: bfloat16 [2048, 6144], replicated
- w2: bfloat16 [6144, 2048], replicated
- norm_moe: bfloat16 [2048], replicated
- wr: bfloat16 [2048, 128], replicated
- ue1: bfloat16 [128, 2048, 768], P('ep')
- ue3: bfloat16 [128, 2048, 768], P('ep')
- ue2: bfloat16 [128, 768, 2048], P('ep')
Outputs:
- output: bfloat16 [8, 256, 2048], P(('dp', 'ep'))
All inputs are finite; a program needn't handle non-finite values.
Results may differ from the reference program's by a relative error of at most 0.0105805.
Values are sent between devices in bfloat16 or wider.
A program may use at most 1 GiB of HBM per device.

```python
import jax
import jax.numpy as jnp
from jax import lax

D = 2048
HEADS = 32
KV_HEADS = 4
HEAD = 128
FF = 6144
EXPERTS = 128
TOP = 8
FE = 768
SEQS_DEV = 1
SEQ = 256
EP = 8

TOKENS = SEQS_DEV * SEQ
CAP = 2 * TOKENS * TOP // EXPERTS
EPS = 1e-6
ROPE_BASE = 10000.0


def _w(key, shape, fan_in, scale=1.0):
    return (scale * fan_in ** -0.5 * jax.random.normal(key, shape, jnp.float32)).astype(jnp.bfloat16)


def _perms(key, count, size):
    return jax.vmap(lambda k: jax.random.permutation(k, size))(jax.random.split(key, count))


def setup_inputs(seed: int = 0, part: int = 0) -> dict:
    key = jax.random.PRNGKey(seed)
    ks = jax.random.split(key, 14)
    kp = jax.random.split(jax.random.fold_in(key, part), 4)
    kd = jax.random.split(jax.random.fold_in(jax.random.fold_in(key, part), 7), 4)
    avg = TOKENS * TOP // EXPERTS
    c = jnp.arange(TOKENS * TOP).reshape(TOKENS, TOP)
    half = TOKENS * TOP // 2
    low = c < half
    e0 = jnp.where(low, c % EXPERTS, (c - half) % (EXPERTS // 2))
    s0 = jnp.where(low, c // EXPERTS, avg // 2 + (c - half) // (EXPERTS // 2))
    shift = jax.random.randint(kd[2], (EP, EXPERTS), 0, CAP)
    tperm = jnp.broadcast_to(_perms(kd[3], EP, TOKENS)[:, :, None], (EP, TOKENS, TOP))
    idx = jnp.take_along_axis(jnp.broadcast_to(e0, (EP, TOKENS, TOP)), tperm, axis=1)
    slot = jnp.take_along_axis((s0[None] + shift[:, e0]) % CAP, tperm, axis=1)
    rshape = (EP * SEQS_DEV, SEQ, TOP)

    def nrm(k):
        return (1.0 + 0.2 * jax.random.normal(k, (D,), jnp.float32)).astype(jnp.bfloat16)

    return {
        'h0': jax.random.normal(kp[0], (EP * SEQS_DEV, SEQ, D), jnp.float32).astype(jnp.bfloat16),
        'idx': idx.reshape(rshape).astype(jnp.int32),
        'slot': slot.reshape(rshape).astype(jnp.int32),
        'norm_attn': nrm(ks[0]),
        'wq': _w(ks[1], (D, HEADS * HEAD), D),
        'wk': _w(ks[2], (D, KV_HEADS * HEAD), D),
        'wv': _w(ks[3], (D, KV_HEADS * HEAD), D),
        'wo': _w(ks[4], (HEADS * HEAD, D), HEADS * HEAD, 2.0),
        'norm_ffn': nrm(ks[5]),
        'w1': _w(ks[6], (D, FF), D),
        'w3': _w(ks[7], (D, FF), D),
        'w2': _w(ks[8], (FF, D), FF, 2.0),
        'norm_moe': nrm(ks[9]),
        'wr': _w(ks[10], (D, EXPERTS), D, 2.0),
        'ue1': _w(ks[11], (EXPERTS, D, FE), D),
        'ue3': _w(ks[12], (EXPERTS, D, FE), D),
        'ue2': _w(ks[13], (EXPERTS, FE, D), FE, 2.0),
    }


def _rms(x, w):
    xf = x.astype(jnp.float32)
    r = lax.rsqrt(jnp.mean(xf * xf, axis=-1, keepdims=True) + EPS)
    return (xf * r * w.astype(jnp.float32)).astype(jnp.bfloat16)


def _rope(x, cos, sin):
    h = HEAD // 2
    x1 = x[..., :h]
    x2 = x[..., h:]
    return jnp.concatenate([x1 * cos - x2 * sin, x2 * cos + x1 * sin], axis=-1)


def _dense_seq(h, na, wq, wk, wv, wo, nf, w1, w3, w2):
    f32 = jnp.float32
    bf = jnp.bfloat16
    pos = jnp.arange(SEQ).astype(f32)
    inv = ROPE_BASE ** (-2.0 * jnp.arange(HEAD // 2).astype(f32) / HEAD)
    ang = pos[:, None] * inv[None, :]
    cos = jnp.cos(ang)[:, None, :]
    sin = jnp.sin(ang)[:, None, :]
    x = _rms(h, na)
    q = _rope(jnp.dot(x, wq, preferred_element_type=f32).reshape(SEQ, HEADS, HEAD), cos, sin).astype(bf)
    k = _rope(jnp.dot(x, wk, preferred_element_type=f32).reshape(SEQ, KV_HEADS, HEAD), cos, sin).astype(bf)
    v = jnp.dot(x, wv, preferred_element_type=f32).astype(bf).reshape(SEQ, KV_HEADS, HEAD)
    q = q.reshape(SEQ, KV_HEADS, HEADS // KV_HEADS, HEAD)
    s = jnp.einsum('qgrd,kgd->grqk', q.astype(f32), k.astype(f32)) * HEAD ** -0.5
    causal = jnp.arange(SEQ)[:, None] >= jnp.arange(SEQ)[None, :]
    s = jnp.where(causal, s, -jnp.inf)
    p = jax.nn.softmax(s, axis=-1).astype(bf)
    o = jnp.einsum('grqk,kgd->qgrd', p.astype(f32), v.astype(f32)).astype(bf).reshape(SEQ, HEADS * HEAD)
    a = (h.astype(f32) + jnp.dot(o, wo, preferred_element_type=f32)).astype(bf)
    z = _rms(a, nf)
    hid = (jax.nn.silu(jnp.dot(z, w1, preferred_element_type=f32)) * jnp.dot(z, w3, preferred_element_type=f32)).astype(bf)
    return a.astype(f32) + jnp.dot(hid, w2, preferred_element_type=f32)


def reference(h0, idx, slot, norm_attn, wq, wk, wv, wo, norm_ffn, w1, w3, w2, norm_moe, wr, ue1, ue3, ue2):
    f32 = jnp.float32
    bf = jnp.bfloat16
    n = EP * TOKENS
    ix = idx.reshape(n, TOP)
    sl = slot.reshape(n, TOP)
    u = _rms(h0.reshape(n, D), norm_moe)
    logits = jnp.dot(u, wr, preferred_element_type=f32)
    g = jax.nn.softmax(jnp.take_along_axis(logits, ix, axis=1), axis=-1)
    rows = jnp.broadcast_to(jnp.arange(n, dtype=jnp.int32)[:, None], (n, TOP))
    src = rows // TOKENS
    tok = jnp.full((EP, EXPERTS, CAP), n, jnp.int32).at[src, ix, sl].set(rows)
    gb = jnp.zeros((EP, EXPERTS, CAP), f32).at[src, ix, sl].set(g)
    tok = tok.transpose(1, 0, 2).reshape(EXPERTS, EP * CAP)
    x = jnp.take(u, tok, axis=0, mode='fill', fill_value=0)

    def expert(args):
        xe, e1, e3, e2 = args
        hid = (jax.nn.silu(jnp.dot(xe, e1, preferred_element_type=f32)) * jnp.dot(xe, e3, preferred_element_type=f32)).astype(bf)
        return jnp.dot(hid, e2, preferred_element_type=f32).astype(bf)

    y = lax.map(expert, (x, ue1, ue3, ue2))
    gw = gb.transpose(1, 0, 2).reshape(EXPERTS, EP * CAP, 1)
    m = jnp.zeros((n, D), f32).at[tok.reshape(-1)].add((gw * y.astype(f32)).reshape(-1, D), mode='drop')
    dense = lax.map(lambda hs: _dense_seq(hs, norm_attn, wq, wk, wv, wo, norm_ffn, w1, w3, w2), h0)
    return (dense + m.reshape(EP * SEQS_DEV, SEQ, D)).astype(bf)
```

```python
import jax
import jax.numpy as jnp
from jax import lax
from jax.sharding import PartitionSpec as P

HEAD = 128
EPS = 1e-6
ROPE_BASE = 10000.0


def _rms(x, w):
    xf = x.astype(jnp.float32)
    r = lax.rsqrt(jnp.mean(xf * xf, axis=-1, keepdims=True) + EPS)
    return (xf * r * w.astype(jnp.float32)).astype(jnp.bfloat16)


def _rope(x, cos, sin):
    h = HEAD // 2
    x1, x2 = x[..., :h], x[..., h:]
    return jnp.concatenate([x1 * cos - x2 * sin, x2 * cos + x1 * sin], axis=-1)


def _dense(h0, na, wq, wk, wv, wo, nf, w1, w3, w2):
    f32, bf = jnp.float32, jnp.bfloat16
    b, s, d = h0.shape
    nh = wq.shape[1] // HEAD
    nkvv = wk.shape[1] // HEAD
    pos = jnp.arange(s).astype(f32)
    inv = ROPE_BASE ** (-2.0 * jnp.arange(HEAD // 2).astype(f32) / HEAD)
    ang = pos[:, None] * inv[None, :]
    cos, sin = jnp.cos(ang)[:, None, :], jnp.sin(ang)[:, None, :]
    x = _rms(h0, na).reshape(b * s, d)
    q = _rope(jnp.dot(x, wq, preferred_element_type=f32).reshape(b, s, nh, HEAD), cos, sin).astype(bf)
    k = _rope(jnp.dot(x, wk, preferred_element_type=f32).reshape(b, s, nkvv, HEAD), cos, sin).astype(bf)
    v = jnp.dot(x, wv, preferred_element_type=f32).astype(bf).reshape(b, s, nkvv, HEAD)
    q = q.reshape(b, s, nkvv, nh // nkvv, HEAD)
    sc = jnp.einsum('bqgrd,bkgd->bgrqk', q, k, preferred_element_type=f32) * HEAD ** -0.5
    causal = jnp.arange(s)[:, None] >= jnp.arange(s)[None, :]
    sc = jnp.where(causal, sc, -jnp.inf)
    p = jax.nn.softmax(sc, axis=-1).astype(bf)
    o = jnp.einsum('bgrqk,bkgd->bqgrd', p, v, preferred_element_type=f32).astype(bf).reshape(b * s, nh * HEAD)
    a = (h0.reshape(b * s, d).astype(f32) + jnp.dot(o, wo, preferred_element_type=f32)).astype(bf)
    z = _rms(a, nf)
    hid = (jax.nn.silu(jnp.dot(z, w1, preferred_element_type=f32)) * jnp.dot(z, w3, preferred_element_type=f32)).astype(bf)
    return a.astype(f32) + jnp.dot(hid, w2, preferred_element_type=f32)


def _experts(x, ue1, ue3, ue2):
    f32 = jnp.float32
    h1 = jnp.einsum('ecd,edf->ecf', x, ue1, preferred_element_type=f32)
    h3 = jnp.einsum('ecd,edf->ecf', x, ue3, preferred_element_type=f32)
    hid = (jax.nn.silu(h1) * h3).astype(jnp.bfloat16)
    return jnp.einsum('ecf,efd->ecd', hid, ue2, preferred_element_type=f32).astype(jnp.bfloat16)


def _split3(g):
    f32, bf = jnp.float32, jnp.bfloat16
    hi = lax.reduce_precision(g, 8, 7)
    r = g - hi
    mid = lax.reduce_precision(r, 8, 7)
    lo = r - mid
    return hi.astype(bf), mid.astype(bf), lo.astype(bf)


def solution(mesh):
    G = mesh.shape['ep']

    def local(h0, idx, slot, na, wq, wk, wv, wo, nf, w1, w3, w2, nm, wr, ue1, ue3, ue2):
        f32, bf = jnp.float32, jnp.bfloat16
        b, s, d = h0.shape
        t = b * s
        k = idx.shape[-1]
        el = ue1.shape[0]
        e = el * G
        cap = 2 * t * k // e
        me = lax.axis_index('ep')
        u = _rms(h0, nm).reshape(t, d)
        meta = jnp.concatenate([idx.reshape(t, k), slot.reshape(t, k)], axis=1).astype(bf)
        meta = jnp.pad(meta, ((0, 0), (0, 128 - 2 * k)))
        allp = lax.all_gather(jnp.concatenate([u, meta], axis=1), 'ep', axis=0, tiled=False)
        ua = allp[..., :d]
        ix = allp[..., d:d + k].astype(jnp.int32)
        sl = allp[..., d + k:d + 2 * k].astype(jnp.int32)
        logits = jnp.einsum('std,de->ste', ua, wr, preferred_element_type=f32)
        onehot = ix[..., None] == jnp.arange(e)
        lg = jnp.sum(jnp.where(onehot, logits[:, :, None, :], 0.0), axis=-1)
        g = jax.nn.softmax(lg, axis=-1)
        key = (ix - me * el) * cap + sl
        key = jnp.where((ix >= me * el) & (ix < (me + 1) * el), key, -1)
        rows = jnp.arange(el * cap)
        hit = key[..., None] == rows
        disp = jnp.any(hit, axis=2).astype(bf)
        gate = jnp.sum(jnp.where(hit, g[..., None], 0.0), axis=2)
        x = jnp.einsum('str,std->rsd', disp, ua, preferred_element_type=f32).astype(bf)
        x = x.reshape(el, cap, G, d).reshape(el, cap * G, d)
        y = _experts(x, ue1, ue3, ue2)
        y = y.reshape(el * cap, G, d)
        m = sum(jnp.einsum('str,rsd->std', p, y, preferred_element_type=f32) for p in _split3(gate))
        m = lax.psum_scatter(m, 'ep', scatter_dimension=0, tiled=False)
        dense = _dense(h0, na, wq, wk, wv, wo, nf, w1, w3, w2)
        return (dense + m).astype(jnp.bfloat16).reshape(b, s, d)

    rows_spec = P(('dp', 'ep'))
    in_specs = (rows_spec,) * 3 + (P(),) * 11 + (P('ep'),) * 3
    return jax.shard_map(local, mesh=mesh, in_specs=in_specs, out_specs=rows_spec, check_vma=False)
```

```python
import jax
import jax.numpy as jnp
from jax import lax
from jax.experimental import pallas as pl
from jax.experimental.pallas import tpu as pltpu
from jax.sharding import PartitionSpec as P

HEAD = 128
EPS = 1e-6
ROPE_BASE = 10000.0
MESH = pl.DeviceIdType.MESH
F32 = jnp.float32
BF = jnp.bfloat16
VMEM_LIMIT = 62 * 1024 * 1024


def _peers():
    me = lax.axis_index('ep')
    core, x, y = me % 2, (me // 2) % 2, me // 4
    out = []
    for r in range(4):
        px = 1 - x if r % 2 else x
        py = 1 - y if r // 2 else y
        for p in range(2):
            pc = 1 - core if p else core
            out.append((py * 2 + px) * 2 + pc)
    return out


def _dot(a, b):
    return jnp.dot(a, b, preferred_element_type=F32)


def _rms_rows(x, w):
    xf = x.astype(F32)
    r = lax.rsqrt(jnp.mean(xf * xf, axis=-1, keepdims=True) + EPS)
    return (xf * r * w.astype(F32)).astype(BF)


def _dispatch(meta, u, e0, cap, rows, x_ref, gt_ref):
    k = meta.shape[0] // 3
    t = meta.shape[1]
    idx, slot, g = meta[:k], meta[k:2 * k], meta[2 * k:3 * k]
    local = idx - e0
    key = jnp.where((local >= 0.0) & (local < rows // cap), local * cap + slot, -1.0)
    step = 128
    for b in range(rows // step):
        row = lax.broadcasted_iota(jnp.int32, (step, t), 0).astype(F32) + float(b * step)
        d = jnp.zeros((step, t), F32)
        gt = jnp.zeros((step, t), F32)
        for j in range(k):
            hit = row == key[j:j + 1, :]
            d = jnp.where(hit, 1.0, d)
            gt = jnp.where(hit, g[j:j + 1, :], gt)
        hi = gt.astype(BF)
        rest = gt - hi.astype(F32)
        mid = rest.astype(BF)
        lo = (rest - mid.astype(F32)).astype(BF)
        gt_ref[0, pl.ds(b * step, step), :] = hi
        gt_ref[0, pl.ds(rows + b * step, step), :] = mid
        gt_ref[0, pl.ds(2 * rows + b * step, step), :] = lo
        x_ref[0, pl.ds(b * step, step), :] = _dot(d.astype(BF), u).astype(BF)


ATT = 8
CH = 4


def _gather_kernel(cap, h0_ref, is_ref, na_ref, nf_ref, nm_ref, cos_ref, sin_ref, wr_ref, wq_ref, wk_ref, wv_ref, wo_ref,
                   x_ref, gt_ref, a_ref, z_ref,
                   u, meta, xa, acc, kb, vb, ob, own_s, own_r, part_s, part_r, fwd_s, fwd_r, rel_s, rel_r, met_s, met_r):
    i = pl.program_id(0)
    peers = _peers()
    t = h0_ref.shape[0]
    rows = x_ref.shape[1]
    hb = wq_ref.shape[1] // HEAD
    ch = t // CH
    order = (tuple(range(CH)), tuple(range(CH // 2, CH)) + tuple(range(CH // 2)))

    def rc(src, dst, ss, rs, peer):
        return pltpu.make_async_remote_copy(src_ref=src, dst_ref=dst, send_sem=ss, recv_sem=rs,
                                            device_id={'ep': peer}, device_id_type=MESH)

    def own(link, n):
        sl = pl.ds(order[link][n] * ch, ch)
        return rc(u.at[0, sl], u.at[2 + 2 * link, sl], own_s.at[link, n], own_r.at[link, n], peers[2 + 2 * link])

    def part():
        return rc(u.at[0], u.at[1], part_s.at[0], part_r.at[0], peers[1])

    def fwd(link, n):
        sl = pl.ds(order[link][n] * ch, ch)
        return rc(u.at[2 + 2 * link, sl], u.at[3 + 2 * link, sl], fwd_s.at[link, n], fwd_r.at[link, n], peers[1])

    def relay(link, n):
        sl = pl.ds(order[link][n] * ch, ch)
        return rc(u.at[2 + 2 * link, sl], u.at[6, sl], rel_s.at[link, n], rel_r.at[link, n], peers[4 - 2 * link])

    def fwd3(link, n):
        sl = pl.ds(order[link][n] * ch, ch)
        return rc(u.at[6, sl], u.at[7, sl], fwd_s.at[2 + link, n], fwd_r.at[2 + link, n], peers[1])

    def met(s):
        return rc(meta.at[0], meta.at[s], met_s.at[s], met_r.at[s], peers[s])

    def pass_on(n):
        for link in range(2):
            own(link, n).wait_recv()
            if n < CH // 2:
                relay(link, n).start()
            fwd(link, n).start()

    @pl.when(i == 0)
    def _():
        barrier = pltpu.get_barrier_semaphore()
        for s in range(1, 8):
            pl.semaphore_signal(barrier, inc=1, device_id={'ep': peers[s]}, device_id_type=MESH)
        uu = _rms_rows(h0_ref[...], nm_ref[...])
        u[0] = uu
        pl.semaphore_wait(barrier, 7)
        for n in range(CH):
            for link in range(2):
                own(link, n).start()
        part().start()
        xa[...] = _rms_rows(h0_ref[...], na_ref[...])
        k = is_ref.shape[0] // 2
        lt = _dot(uu, wr_ref[...]).T
        it = is_ref[...]
        ids = lax.broadcasted_iota(jnp.int32, lt.shape, 0)
        sel = [jnp.sum(jnp.where(ids == it[j:j + 1, :], lt, 0.0), axis=0, keepdims=True) for j in range(k)]
        lg = jnp.concatenate(sel, axis=0)
        ex = jnp.exp(lg - jnp.max(lg, axis=0, keepdims=True))
        meta[0, 0:2 * k, :] = it.astype(F32)
        meta[0, 2 * k:3 * k, :] = ex / jnp.sum(ex, axis=0, keepdims=True)
        acc[...] = h0_ref[...].astype(F32)

    @pl.when(i == 1)
    def _():
        for s in range(1, 8):
            met(s).start()

    @pl.when(i < ATT)
    def _():
        x = xa[...]
        cos, sin = cos_ref[...], sin_ref[...]

        def rope(v):
            return (v * cos + pltpu.roll(v, HEAD // 2, 1) * sin).astype(BF)

        @pl.when(i % 2 == 0)
        def _():
            kb[...] = rope(_dot(x, wk_ref[...]))
            vb[...] = _dot(x, wv_ref[...]).astype(BF)

        q = _dot(x, wq_ref[...])
        causal = lax.broadcasted_iota(jnp.int32, (t, t), 0) >= lax.broadcasted_iota(jnp.int32, (t, t), 1)
        kk, vv = kb[...], vb[...]
        for h in range(hb):
            qh = rope(q[:, h * HEAD:(h + 1) * HEAD])
            s = lax.dot_general(qh, kk, (((1,), (1,)), ((), ())), preferred_element_type=F32) * HEAD ** -0.5
            s = jnp.where(causal, s, -jnp.inf)
            ex = jnp.exp(s - jnp.max(s, axis=1, keepdims=True))
            p = (ex / jnp.sum(ex, axis=1, keepdims=True)).astype(BF)
            ob[:, h * HEAD:(h + 1) * HEAD] = _dot(p, vv).astype(BF)
        acc[...] += _dot(ob[...], wo_ref[...])

    for n in range(CH):
        @pl.when(i == 2 * n + 2)
        def _(n=n):
            pass_on(n)

    @pl.when(i == ATT)
    def _():
        a = acc[...].astype(BF)
        a_ref[...] = a
        z_ref[...] = _rms_rows(a, nf_ref[...])

    for s in range(8):
        @pl.when(i == ATT + s)
        def _(s=s):
            if s == 1:
                part().wait_recv()
            if s in (3, 5):
                for n in range(CH):
                    fwd((s - 3) // 2, n).wait_recv()
            if s == 6:
                for n in range(CH // 2):
                    for link in range(2):
                        relay(link, n).wait_recv()
                        fwd3(link, n).start()
            if s == 7:
                for n in range(CH // 2):
                    for link in range(2):
                        fwd3(link, n).wait_recv()
            if s:
                met(s).wait_recv()
            e0 = lax.axis_index('ep') * (rows // cap)
            _dispatch(meta[s], u[s], e0.astype(F32), cap, rows, x_ref, gt_ref)
            if s == 7:
                part().wait_send()
                for link in range(2):
                    for n in range(CH):
                        own(link, n).wait_send()
                        fwd(link, n).wait_send()
                        if n < CH // 2:
                            relay(link, n).wait_send()
                            fwd3(link, n).wait_send()
                for q in range(1, 8):
                    met(q).wait_send()


def _gather(h0, ist, na, nf, nm, cos, sin, wr, wq, wk, wv, wo, el, cap):
    t, d = h0.shape
    rows = el * cap
    qb = wq.shape[1] // ATT
    kv = wk.shape[1] // HEAD
    full = lambda a: pl.BlockSpec(a.shape, lambda i: (0,) * a.ndim)
    att = lambda i: jnp.minimum(i, ATT - 1)
    src = lambda i: jnp.maximum(i - ATT, 0)
    dma = pltpu.SemaphoreType.DMA
    return pl.pallas_call(
        lambda *refs: _gather_kernel(cap, *refs),
        grid=(ATT + 8,),
        in_specs=[full(h0), full(ist), full(na), full(nf), full(nm), full(cos), full(sin), full(wr),
                  pl.BlockSpec((d, qb), lambda i: (0, att(i))),
                  pl.BlockSpec((d, HEAD), lambda i: (0, att(i) * kv // ATT)),
                  pl.BlockSpec((d, HEAD), lambda i: (0, att(i) * kv // ATT)),
                  pl.BlockSpec((qb, d), lambda i: (att(i), 0))],
        out_specs=[pl.BlockSpec((1, rows, d), lambda i: (src(i), 0, 0)),
                   pl.BlockSpec((1, 3 * rows, t), lambda i: (src(i), 0, 0)),
                   pl.BlockSpec((t, d), lambda i: (0, 0)), pl.BlockSpec((t, d), lambda i: (0, 0))],
        out_shape=[jax.ShapeDtypeStruct((8, rows, d), BF), jax.ShapeDtypeStruct((8, 3 * rows, t), BF),
                   jax.ShapeDtypeStruct((t, d), BF), jax.ShapeDtypeStruct((t, d), BF)],
        scratch_shapes=[pltpu.VMEM((8, t, d), BF), pltpu.VMEM((8, 3 * ist.shape[0] // 2, t), F32),
                        pltpu.VMEM((t, d), BF), pltpu.VMEM((t, d), F32),
                        pltpu.VMEM((t, HEAD), BF), pltpu.VMEM((t, HEAD), BF), pltpu.VMEM((t, qb), BF),
                        dma((2, CH)), dma((2, CH)), dma((1,)), dma((1,)), dma((4, CH)), dma((4, CH)),
                        dma((2, CH)), dma((2, CH)), dma((8,)), dma((8,))],
        compiler_params=pltpu.CompilerParams(dimension_semantics=('arbitrary',), collective_id=0, has_side_effects=True,
                                             vmem_limit_bytes=VMEM_LIMIT),
        name='gather_attention',
    )(h0, ist, na, nf, nm, cos, sin, wr, wq, wk, wv, wo)


def _up_kernel(x_ref, w1_ref, w3_ref, o_ref):
    x = x_ref[...].reshape(o_ref.shape[1], x_ref.shape[-1])
    h1 = _dot(x, w1_ref[0])
    h3 = _dot(x, w3_ref[0])
    o_ref[0] = (h1 * jax.nn.sigmoid(h1) * h3).astype(BF)


def _up(x, ue1, ue3, cap):
    el, d, fe = ue1.shape
    m = 8 * cap
    w = pl.BlockSpec((1, d, fe), lambda e: (e, 0, 0))
    return pl.pallas_call(
        _up_kernel,
        grid=(el,),
        in_specs=[pl.BlockSpec((8, 1, cap, d), lambda e: (0, e, 0, 0)), w, w],
        out_specs=pl.BlockSpec((1, m, fe), lambda e: (e, 0, 0)),
        out_shape=jax.ShapeDtypeStruct((el, m, fe), BF),
        compiler_params=pltpu.CompilerParams(dimension_semantics=('arbitrary',), vmem_limit_bytes=VMEM_LIMIT),
        name='expert_up',
    )(x.reshape(8, el, cap, d), ue1, ue3)


NC = 8
FS = 24
FLAG = 2
LANES = 128
POS = ((0, 2, 1, 3), (0, 1, 2, 3))


def _down_kernel(cap, hid_ref, gt_ref, a_ref, z_ref, ue2_ref, w1_ref, w3_ref, w2_ref, out_ref,
                 yb, mo, mp, r0, r1, r2, acc, d_s, d_r, credit, p1_s, p1_r, p2_s, p2_r):
    i = pl.program_id(0)
    peers = _peers()
    el, m, fe = hid_ref.shape
    half = ue2_ref.shape[0]
    rows = el * cap

    def rc(src, dst, ss, rs, peer):
        return pltpu.make_async_remote_copy(src_ref=src, dst_ref=dst, send_sem=ss, recv_sem=rs,
                                            device_id={'ep': peer}, device_id_type=MESH)

    def pair(c):
        return rc(mo.at[c % 2], r0.at[c % 2], d_s.at[c % 2], d_r.at[c % 2], peers[1])

    def first(c, b):
        return rc(mp.at[c, b, pl.ds(2, 2)], r1.at[c, b], p1_s.at[c, b], p1_r.at[c, b], peers[2 + 2 * b])

    def second(c, b):
        return rc(mp.at[c, b, 1], r2.at[c, b], p2_s.at[c, b], p2_r.at[c, b], peers[4 - 2 * b])

    @pl.when(i == 0)
    def _():
        barrier = pltpu.get_barrier_semaphore()
        for s in (1, 2, 4):
            pl.semaphore_signal(barrier, inc=1, device_id={'ep': peers[s]}, device_id_type=MESH)
        acc[...] = a_ref[...].astype(F32)
        pl.semaphore_wait(barrier, 3)

    @pl.when(i < 2 * NC)
    def _():
        base = (i % 2) * half
        for e in range(half):
            y = _dot(hid_ref[base + e], ue2_ref[e]).astype(BF)
            for s in range(8):
                yb[s, pl.ds(pl.multiple_of((base + e) * cap, cap), cap), :] = y[s * cap:(s + 1) * cap]

    @pl.when((i % 2 == 0) & (i >= 2) & (i <= 2 * NC))
    def _():
        c = i // 2 - 1
        pair(c).wait()
        mp[c] = mp[c] + r0[c % 2]

        @pl.when(c < NC - 2)
        def _():
            pl.semaphore_signal(credit, inc=1, device_id={'ep': peers[1]}, device_id_type=MESH)

        for b in range(2):
            first(c, b).start()

    @pl.when((i % 2 == 1) & (i < 2 * NC))
    def _():
        c = i // 2
        for s in range(8):
            y = yb[s]
            v = None
            for q in range(3):
                w = lax.dot_general(gt_ref[s, pl.ds(q * rows, rows), :], y, (((0,), (0,)), ((), ())),
                                    preferred_element_type=F32)
                v = w if v is None else v + w
            for b in range(2):
                dst = v[:, b * LANES:(b + 1) * LANES]
                if s % 2:
                    mo[c % 2, b, POS[b][s // 2]] = dst
                else:
                    mp[c, b, POS[b][s // 2]] = dst

        @pl.when(c >= 2)
        def _():
            pl.semaphore_wait(credit, 1)

        pair(c).start()

    @pl.when(i >= FLAG)
    def _():
        z = z_ref[...]
        h1 = _dot(z, w1_ref[...])
        h3 = _dot(z, w3_ref[...])
        acc[...] += _dot((h1 * jax.nn.sigmoid(h1) * h3).astype(BF), w2_ref[...])

    @pl.when((i % 2 == 1) & (i >= 5) & (i < 2 * NC + 5))
    def _():
        c = (i - 5) // 2
        for b in range(2):
            first(c, b).wait_recv()
            mp[c, b, pl.ds(0, 2)] = mp[c, b, pl.ds(0, 2)] + r1[c, b]
            second(c, b).start()

    @pl.when(i == FS + FLAG - 1)
    def _():
        for c in range(NC):
            for b in range(2):
                second(c, b).wait_recv()
                col = pl.ds((2 * c + b) * LANES, LANES)
                out_ref[:, col] = (acc[:, col] + (mp[c, b, 0] + r2[c, b])).astype(BF)
        for c in range(NC):
            for b in range(2):
                first(c, b).wait_send()
                second(c, b).wait_send()


def _down(hid, gt, a, z, ue2, w1, w3, w2, cap):
    el, m, fe = hid.shape
    t, d = a.shape
    nb = d // NC
    fb = w1.shape[1] // FS
    full = lambda v: pl.BlockSpec(v.shape, lambda i: (0,) * v.ndim, pipeline_mode=pl.Buffered(1))
    ci = lambda i: jnp.minimum(i, 2 * NC - 1)
    fi = lambda i: jnp.clip(i - FLAG, 0, FS - 1)
    dma = pltpu.SemaphoreType.DMA
    return pl.pallas_call(
        lambda *refs: _down_kernel(cap, *refs),
        grid=(FS + FLAG,),
        in_specs=[full(hid), full(gt), full(a), full(z),
                  pl.BlockSpec((el // 2, fe, nb), lambda i: (ci(i) % 2, 0, ci(i) // 2)),
                  pl.BlockSpec((d, fb), lambda i: (0, fi(i))),
                  pl.BlockSpec((d, fb), lambda i: (0, fi(i))),
                  pl.BlockSpec((fb, d), lambda i: (fi(i), 0))],
        out_specs=pl.BlockSpec((t, d), lambda i: (0, 0)),
        out_shape=jax.ShapeDtypeStruct((t, d), BF),
        scratch_shapes=[pltpu.VMEM((8, el * cap, nb), BF),
                        pltpu.VMEM((2, 2, 4, t, LANES), F32), pltpu.VMEM((NC, 2, 4, t, LANES), F32),
                        pltpu.VMEM((2, 2, 4, t, LANES), F32), pltpu.VMEM((NC, 2, 2, t, LANES), F32),
                        pltpu.VMEM((NC, 2, t, LANES), F32), pltpu.VMEM((t, d), F32),
                        dma((2,)), dma((2,)), pltpu.SemaphoreType.REGULAR,
                        dma((NC, 2)), dma((NC, 2)), dma((NC, 2)), dma((NC, 2))],
        compiler_params=pltpu.CompilerParams(dimension_semantics=('arbitrary',), collective_id=1, has_side_effects=True,
                                             vmem_limit_bytes=VMEM_LIMIT),
        name='expert_down_ffn',
    )(hid, gt, a, z, ue2, w1, w3, w2)


def solution(mesh):
    G = mesh.shape['ep']

    def local(h0, idx, slot, na, wq, wk, wv, wo, nf, w1, w3, w2, nm, wr, ue1, ue3, ue2):
        b, s, d = h0.shape
        k = idx.shape[-1]
        el = ue1.shape[0]
        cap = 2 * s * k // (el * G)
        pos = jnp.arange(s).astype(F32)
        inv = ROPE_BASE ** (-2.0 * jnp.arange(HEAD // 2).astype(F32) / HEAD)
        ang = pos[:, None] * inv[None, :]
        cos, sin = jnp.cos(ang), jnp.sin(ang)
        cos = jnp.concatenate([cos, cos], axis=1)
        sin = jnp.concatenate([-sin, sin], axis=1)
        ist = jnp.concatenate([idx.reshape(s, k).T, slot.reshape(s, k).T], axis=0)
        h = h0.reshape(s, d)
        x, gt, a, z = _gather(h, ist, na.reshape(1, d), nf.reshape(1, d), nm.reshape(1, d), cos, sin, wr, wq, wk, wv, wo,
                              el, cap)
        hid = _up(x, ue1, ue3, cap)
        return _down(hid, gt, a, z, ue2, w1, w3, w2, cap).reshape(b, s, d)

    rows_spec = P(('dp', 'ep'))
    in_specs = (rows_spec,) * 3 + (P(),) * 11 + (P('ep'),) * 3
    return jax.shard_map(local, mesh=mesh, in_specs=in_specs, out_specs=rows_spec, check_vma=False)
```

```python
import jax
import jax.numpy as jnp
import numpy as np
from jax import lax
from jax.experimental import pallas as pl
from jax.experimental.pallas import tpu as pltpu
from jax.sharding import PartitionSpec as P

HEAD = 128
EPS = 1e-6
ROPE_BASE = 10000.0
MESH = pl.DeviceIdType.MESH
F32 = jnp.float32
BF = jnp.bfloat16
VMEM_LIMIT = 62 * 1024 * 1024


def _peers():
    me = lax.axis_index('ep')
    core, x, y = me % 2, (me // 2) % 2, me // 4
    out = []
    for r in range(4):
        px = 1 - x if r % 2 else x
        py = 1 - y if r // 2 else y
        for p in range(2):
            pc = 1 - core if p else core
            out.append((py * 2 + px) * 2 + pc)
    return out


def _tables(t):
    inv = ROPE_BASE ** (-2.0 * np.arange(HEAD // 2, dtype=np.float64) / HEAD)
    ang = np.arange(t, dtype=np.float64)[:, None] * inv[None, :]
    cos, sin = np.cos(ang), np.sin(ang)
    return (jnp.asarray(np.concatenate([cos, cos], axis=1), F32), jnp.asarray(np.concatenate([-sin, sin], axis=1), F32))


def _dot(a, b):
    return jnp.dot(a, b, preferred_element_type=F32)


def _rms_rows(x, w):
    xf = x.astype(F32)
    r = lax.rsqrt(jnp.mean(xf * xf, axis=-1, keepdims=True) + EPS)
    return (xf * r * w.astype(F32)).astype(BF)


def _dispatch(meta, u, e0, cap, rows, x_ref, gt_ref):
    k = meta.shape[0] // 3
    t = meta.shape[1]
    idx, slot, g = meta[:k], meta[k:2 * k], meta[2 * k:3 * k]
    local = idx - e0
    key = jnp.where((local >= 0.0) & (local < rows // cap), local * cap + slot, -1.0)
    step = 128
    for b in range(rows // step):
        row = lax.broadcasted_iota(jnp.int32, (step, t), 0).astype(F32) + float(b * step)
        d = jnp.zeros((step, t), F32)
        gt = jnp.zeros((step, t), F32)
        for j in range(k):
            hit = row == key[j:j + 1, :]
            d = jnp.where(hit, 1.0, d)
            gt = jnp.where(hit, g[j:j + 1, :], gt)
        col = pl.ds(b * step, step)
        gt = gt.T
        hi = gt.astype(BF)
        rest = gt - hi.astype(F32)
        mid = rest.astype(BF)
        lo = (rest - mid.astype(F32)).astype(BF)
        gt_ref[0:t, col] = hi
        gt_ref[t:2 * t, col] = mid
        gt_ref[2 * t:3 * t, col] = lo
        x_ref[pl.ds(b * step, step), :] = _dot(d.astype(BF), u).astype(BF)


ATT = 8
CH = 4
RING = 3
PASS = (3, 6, 9, 11)
D0 = ATT + 1
E0 = D0 + 8


def _front_kernel(cap, h0_ref, ix_ref, sl_ref, na_ref, nm_ref, cos_ref, sin_ref, wr_ref, wq_ref, wk_ref, wv_ref,
                  wo_ref, ue1_ref, ue3_ref, hid_ref, gt_ref, a_ref,
                  u, meta, acc, kb, vb, xs, ring, own_s, own_r, part_s, part_r, fwd_s, fwd_r, rel_s, rel_r,
                  met_s, met_r, ring_s):
    i = pl.program_id(0)
    peers = _peers()
    t, d = h0_ref.shape
    rows = xs.shape[1]
    el = rows // cap
    hb = wq_ref.shape[1] // HEAD
    ch = t // CH
    order = (tuple(range(CH)), tuple(range(CH // 2, CH)) + tuple(range(CH // 2)))

    def rc(src, dst, ss, rs, peer):
        return pltpu.make_async_remote_copy(src_ref=src, dst_ref=dst, send_sem=ss, recv_sem=rs,
                                            device_id={'ep': peer}, device_id_type=MESH)

    def own(link, n):
        sl = pl.ds(order[link][n] * ch, ch)
        return rc(u.at[0, sl], u.at[2 + 2 * link, sl], own_s.at[link, n], own_r.at[link, n], peers[2 + 2 * link])

    def part():
        return rc(u.at[0], u.at[1], part_s.at[0], part_r.at[0], peers[1])

    def fwd(link, n):
        sl = pl.ds(order[link][n] * ch, ch)
        return rc(u.at[2 + 2 * link, sl], u.at[3 + 2 * link, sl], fwd_s.at[link, n], fwd_r.at[link, n], peers[1])

    def relay(link, n):
        sl = pl.ds(order[link][n] * ch, ch)
        return rc(u.at[2 + 2 * link, sl], u.at[6, sl], rel_s.at[link, n], rel_r.at[link, n], peers[4 - 2 * link])

    def fwd3(link, n):
        sl = pl.ds(order[link][n] * ch, ch)
        return rc(u.at[6, sl], u.at[7, sl], fwd_s.at[2 + link, n], fwd_r.at[2 + link, n], peers[1])

    def met(s):
        return rc(meta.at[0], meta.at[s], met_s.at[s], met_r.at[s], peers[s])

    def weights(e, j):
        return pltpu.make_async_copy((ue1_ref, ue3_ref)[j].at[e], ring.at[e % RING, j], ring_s.at[e % RING, j])

    def pass_on(n):
        for link in range(2):
            own(link, n).wait_recv()
            if n < CH // 2:
                relay(link, n).start()
            fwd(link, n).start()

    @pl.when(i == 0)
    def _():
        barrier = pltpu.get_barrier_semaphore()
        for s in range(1, 8):
            pl.semaphore_signal(barrier, inc=1, device_id={'ep': peers[s]}, device_id_type=MESH)
        uu = _rms_rows(h0_ref[...], nm_ref[...])
        u[0] = uu
        pl.semaphore_wait(barrier, 7)
        for n in range(CH):
            for link in range(2):
                own(link, n).start()
        part().start()
        for e in range(RING):
            for j in range(2):
                weights(e, j).start()
        xs[7, 0:t] = _rms_rows(h0_ref[...], na_ref[...])
        k = ix_ref.shape[1]
        lt = _dot(uu, wr_ref[...]).T
        it = ix_ref[0]
        ids = lax.broadcasted_iota(jnp.int32, lt.shape, 0)
        sel = [jnp.sum(jnp.where(ids == it[j:j + 1, :], lt, 0.0), axis=0, keepdims=True) for j in range(k)]
        lg = jnp.concatenate(sel, axis=0)
        ex = jnp.exp(lg - jnp.max(lg, axis=0, keepdims=True))
        meta[0, 0:k, :] = it.astype(F32)
        meta[0, k:2 * k, :] = sl_ref[0].astype(F32)
        meta[0, 2 * k:3 * k, :] = ex / jnp.sum(ex, axis=0, keepdims=True)
        acc[...] = h0_ref[...].astype(F32)

    @pl.when(i == 1)
    def _():
        for s in range(1, 8):
            met(s).start()

    for n in range(CH):
        @pl.when(i == PASS[n])
        def _(n=n):
            pass_on(n)

    def rope(v):
        return (v * cos_ref[...] + pltpu.roll(v, HEAD // 2, 1) * sin_ref[...]).astype(BF)

    def project():
        q = _dot(xs[7, 0:t], wq_ref[...])

        def finish():
            for h in range(hb):
                xs[6 + i % 2, t:2 * t, h * HEAD:(h + 1) * HEAD] = rope(q[:, h * HEAD:(h + 1) * HEAD])
        return finish

    def keys():
        g = (i // 2) % 2
        kb[g] = rope(_dot(xs[7, 0:t], wk_ref[...]))
        vb[g] = _dot(xs[7, 0:t], wv_ref[...]).astype(BF)

    def attend(between):
        g = ((i - 1) // 2) % 2
        kk, vv = kb[g], vb[g]
        causal = lax.broadcasted_iota(jnp.int32, (t, t), 0) >= lax.broadcasted_iota(jnp.int32, (t, t), 1)
        sc = [lax.dot_general(xs[6 + (i - 1) % 2, t:2 * t, h * HEAD:(h + 1) * HEAD], kk, (((1,), (1,)), ((), ())),
                              preferred_element_type=F32) for h in range(hb)]
        finish = between()
        o = []
        for h in range(hb):
            s = jnp.where(causal, sc[h] * HEAD ** -0.5, -jnp.inf)
            ex = jnp.exp(s - jnp.max(s, axis=1, keepdims=True))
            p = (ex / jnp.sum(ex, axis=1, keepdims=True)).astype(BF)
            o.append(_dot(p, vv).astype(BF))
        finish()
        acc[...] += _dot(jnp.concatenate(o, axis=1), wo_ref[...])

    @pl.when((i < ATT) & (i % 2 == 0))
    def _():
        keys()

    @pl.when(i == 0)
    def _():
        project()()

    @pl.when((i >= 1) & (i < ATT))
    def _():
        attend(project)

    @pl.when(i == ATT)
    def _():
        attend(lambda: lambda: None)
        a_ref[...] = acc[...].astype(BF)

    for s in range(8):
        @pl.when(i == D0 + s)
        def _(s=s):
            if s == 1:
                part().wait_recv()
            if s in (3, 5):
                for n in range(CH):
                    fwd((s - 3) // 2, n).wait_recv()
            if s == 6:
                for n in range(CH // 2):
                    for link in range(2):
                        relay(link, n).wait_recv()
                        fwd3(link, n).start()
            if s == 7:
                for n in range(CH // 2):
                    for link in range(2):
                        fwd3(link, n).wait_recv()
            if s:
                met(s).wait_recv()
            e0 = lax.axis_index('ep') * el
            _dispatch(meta[s], u[s], e0.astype(F32), cap, rows, xs.at[s], gt_ref.at[0])

    @pl.when(i >= E0)
    def _():
        e = i - E0
        for j in range(2):
            weights(e, j).wait()
        x = xs[:, pl.ds(pl.multiple_of(e * cap, cap), cap), :].reshape(8 * cap, d)
        h1 = _dot(x, ring[e % RING, 0])
        h3 = _dot(x, ring[e % RING, 1])
        hid_ref[0] = (h1 * jax.nn.sigmoid(h1) * h3).astype(BF)

        @pl.when(e < el - RING)
        def _():
            for j in range(2):
                weights(e + RING, j).start()

    @pl.when(i == E0 + el - 1)
    def _():
        part().wait_send()
        for link in range(2):
            for n in range(CH):
                own(link, n).wait_send()
                fwd(link, n).wait_send()
                if n < CH // 2:
                    relay(link, n).wait_send()
                    fwd3(link, n).wait_send()
        for q in range(1, 8):
            met(q).wait_send()


def _front(h0, idx, slot, na, nm, cos, sin, wr, wq, wk, wv, wo, ue1, ue3, cap):
    t, d = h0.shape
    el, _, fe = ue1.shape
    rows = el * cap
    qb = wq.shape[1] // ATT
    kv = wk.shape[1] // HEAD
    full = lambda a: pl.BlockSpec(a.shape, lambda i: (0,) * a.ndim, pipeline_mode=pl.Buffered(1))
    one = pl.BlockSpec((t, d), lambda i: (0, 0), pipeline_mode=pl.Buffered(1))
    att = lambda i: jnp.minimum(i, ATT - 1)
    prev = lambda i: jnp.clip(i - 1, 0, ATT - 1)
    src = lambda i: jnp.clip(i - D0, 0, 7)
    hbm = pl.BlockSpec(memory_space=pl.ANY)
    dma = pltpu.SemaphoreType.DMA
    return pl.pallas_call(
        lambda *refs: _front_kernel(cap, *refs),
        grid=(E0 + el,),
        in_specs=[full(h0), full(idx), full(slot), full(na), full(nm), full(cos), full(sin), full(wr),
                  pl.BlockSpec((d, qb), lambda i: (0, att(i))),
                  pl.BlockSpec((d, HEAD), lambda i: (0, att(i) * kv // ATT)),
                  pl.BlockSpec((d, HEAD), lambda i: (0, att(i) * kv // ATT)),
                  pl.BlockSpec((qb, d), lambda i: (prev(i), 0)), hbm, hbm],
        out_specs=[pl.BlockSpec((1, 8 * cap, fe), lambda i: (jnp.maximum(i - E0, 0), 0, 0)),
                   pl.BlockSpec((1, 3 * t, rows), lambda i: (src(i), 0, 0)), one],
        out_shape=[jax.ShapeDtypeStruct((el, 8 * cap, fe), BF), jax.ShapeDtypeStruct((8, 3 * t, rows), BF),
                   jax.ShapeDtypeStruct((t, d), BF)],
        scratch_shapes=[pltpu.VMEM((8, t, d), BF), pltpu.VMEM((8, 3 * idx.shape[1], t), F32),
                        pltpu.VMEM((t, d), F32),
                        pltpu.VMEM((2, t, HEAD), BF), pltpu.VMEM((2, t, HEAD), BF),
                        pltpu.VMEM((8, rows, d), BF), pltpu.VMEM((RING, 2, d, fe), BF),
                        dma((2, CH)), dma((2, CH)), dma((1,)), dma((1,)), dma((4, CH)), dma((4, CH)),
                        dma((2, CH)), dma((2, CH)), dma((8,)), dma((8,)), dma((RING, 2))],
        compiler_params=pltpu.CompilerParams(dimension_semantics=('arbitrary',), collective_id=0, has_side_effects=True,
                                             vmem_limit_bytes=67043328),
        name='gather_attention_up',
    )(h0, idx, slot, na, nm, cos, sin, wr, wq, wk, wv, wo, ue1, ue3)


NC = 8
FS = 16
LANES = 128
POS = ((0, 2, 1, 3), (0, 1, 2, 3))


def _down_kernel(cap, hid_ref, gt_ref, a_ref, nf_ref, ue2_ref, w1_ref, w3_ref, w2_ref, out_ref,
                 zb, yb, mo, mp, r0, r1, r2, acc, d_s, d_r, credit, p1_s, p1_r, p2_s, p2_r):
    i = pl.program_id(0)
    peers = _peers()
    el, m, fe = hid_ref.shape
    t = a_ref.shape[0]

    def rc(src, dst, ss, rs, peer):
        return pltpu.make_async_remote_copy(src_ref=src, dst_ref=dst, send_sem=ss, recv_sem=rs,
                                            device_id={'ep': peer}, device_id_type=MESH)

    def pair(c):
        return rc(mo.at[c % 2], r0.at[c % 2], d_s.at[c % 2], d_r.at[c % 2], peers[1])

    def first(c, b):
        return rc(mp.at[c, b, pl.ds(2, 2)], r1.at[c, b], p1_s.at[c, b], p1_r.at[c, b], peers[2 + 2 * b])

    def second(c, b):
        return rc(mp.at[c, b, 1], r2.at[c, b], p2_s.at[c, b], p2_r.at[c, b], peers[4 - 2 * b])

    def second_step(c):
        for b in range(2):
            first(c, b).wait_recv()
            mp[c, b, pl.ds(0, 2)] = mp[c, b, pl.ds(0, 2)] + r1[c, b]
            second(c, b).start()

    def ffn_up():
        z = zb[...]
        h1 = _dot(z, w1_ref[...])
        h3 = _dot(z, w3_ref[...])
        return (h1 * jax.nn.sigmoid(h1) * h3).astype(BF)

    @pl.when(i == 0)
    def _():
        barrier = pltpu.get_barrier_semaphore()
        for s in (1, 2, 4):
            pl.semaphore_signal(barrier, inc=1, device_id={'ep': peers[s]}, device_id_type=MESH)
        acc[...] = a_ref[...].astype(F32)
        zb[...] = _rms_rows(a_ref[...], nf_ref[...])
        pl.semaphore_wait(barrier, 3)

    @pl.when((i >= 1) & (i <= NC))
    def _():
        c = i - 1
        pair(c).wait()
        mp[c] = mp[c] + r0[c % 2]

        @pl.when(c < NC - 2)
        def _():
            pl.semaphore_signal(credit, inc=1, device_id={'ep': peers[1]}, device_id_type=MESH)

        for b in range(2):
            first(c, b).start()

    @pl.when((i >= 2) & (i < NC))
    def _():
        pl.semaphore_wait(credit, 1)

    @pl.when((i >= LAG) & (i < NC))
    def _():
        second_step(i - LAG)

    for c in range(NC - LAG, NC):
        @pl.when(i == NC + 1 + LATE * (c - NC + LAG))
        def _(c=c):
            second_step(c)

    @pl.when(i < NC)
    def _():
        for e in range(el):
            y = _dot(hid_ref[e], ue2_ref[e]).astype(BF)
            for s in range(8):
                yb[s, e * cap:(e + 1) * cap, :] = y[s * cap:(s + 1) * cap]
        hf = ffn_up()
        for s in range(8):
            v = _dot(gt_ref[s], yb[s])
            v = v[:t] + v[t:2 * t] + v[2 * t:]
            for b in range(2):
                dst = v[:, b * LANES:(b + 1) * LANES]
                if s % 2:
                    mo[i % 2, b, POS[b][s // 2]] = dst
                else:
                    mp[i, b, POS[b][s // 2]] = dst
        pair(i).start()
        acc[...] += _dot(hf, w2_ref[...])

    @pl.when(i >= NC)
    def _():
        acc[...] += _dot(ffn_up(), w2_ref[...])

    @pl.when(i == FS - 1)
    def _():
        for c in range(NC):
            for b in range(2):
                second(c, b).wait_recv()
                col = pl.ds((2 * c + b) * LANES, LANES)
                out_ref[:, col] = (acc[:, col] + (mp[c, b, 0] + r2[c, b])).astype(BF)
        for c in range(NC):
            for b in range(2):
                first(c, b).wait_send()
                second(c, b).wait_send()


LAG = 3
LATE = 2


def _down(hid, gt, a, nf, ue2, w1, w3, w2, cap):
    el, m, fe = hid.shape
    t, d = a.shape
    nb = d // NC
    fb = w1.shape[1] // FS
    full = lambda v: pl.BlockSpec(v.shape, lambda i: (0,) * v.ndim, pipeline_mode=pl.Buffered(1))
    dma = pltpu.SemaphoreType.DMA
    return pl.pallas_call(
        lambda *refs: _down_kernel(cap, *refs),
        grid=(FS,),
        in_specs=[full(hid), full(gt), full(a), full(nf),
                  pl.BlockSpec((el, fe, nb), lambda i: (0, 0, jnp.minimum(i, NC - 1))),
                  pl.BlockSpec((d, fb), lambda i: (0, i)),
                  pl.BlockSpec((d, fb), lambda i: (0, i)),
                  pl.BlockSpec((fb, d), lambda i: (i, 0))],
        out_specs=pl.BlockSpec((t, d), lambda i: (0, 0), pipeline_mode=pl.Buffered(1)),
        out_shape=jax.ShapeDtypeStruct((t, d), BF),
        scratch_shapes=[pltpu.VMEM((t, d), BF), pltpu.VMEM((8, el * cap, nb), BF),
                        pltpu.VMEM((2, 2, 4, t, LANES), F32), pltpu.VMEM((NC, 2, 4, t, LANES), F32),
                        pltpu.VMEM((2, 2, 4, t, LANES), F32), pltpu.VMEM((NC, 2, 2, t, LANES), F32),
                        pltpu.VMEM((NC, 2, t, LANES), F32), pltpu.VMEM((t, d), F32),
                        dma((2,)), dma((2,)), pltpu.SemaphoreType.REGULAR,
                        dma((NC, 2)), dma((NC, 2)), dma((NC, 2)), dma((NC, 2))],
        compiler_params=pltpu.CompilerParams(dimension_semantics=('arbitrary',), collective_id=1, has_side_effects=True,
                                             vmem_limit_bytes=67043328),
        name='expert_down_ffn',
    )(hid, gt, a, nf, ue2, w1, w3, w2)


def solution(mesh):
    G = mesh.shape['ep']

    def local(h0, idx, slot, na, wq, wk, wv, wo, nf, w1, w3, w2, nm, wr, ue1, ue3, ue2):
        b, s, d = h0.shape
        k = idx.shape[-1]
        el = ue1.shape[0]
        cap = 2 * s * k // (el * G)
        cos, sin = _tables(s)
        h = h0.reshape(s, d)
        hid, gt, a = _front(h, jnp.swapaxes(idx, 1, 2), jnp.swapaxes(slot, 1, 2), na, nm, cos, sin, wr, wq, wk, wv,
                               wo, ue1, ue3, cap)
        return _down(hid, gt, a, nf, ue2, w1, w3, w2, cap).reshape(b, s, d)

    rows_spec = P(('dp', 'ep'))
    in_specs = (rows_spec,) * 3 + (P(),) * 11 + (P('ep'),) * 3
    return jax.shard_map(local, mesh=mesh, in_specs=in_specs, out_specs=rows_spec, check_vma=False)
```

```python
import jax
import jax.numpy as jnp
import numpy as np
from jax import lax
from jax.experimental import pallas as pl
from jax.experimental.pallas import tpu as pltpu
from jax.sharding import PartitionSpec as P

HEAD = 128
EPS = 1e-6
ROPE_BASE = 10000.0
MESH = pl.DeviceIdType.MESH
F32 = jnp.float32
BF = jnp.bfloat16
VMEM_LIMIT = 62 * 1024 * 1024


def _peers():
    me = lax.axis_index('ep')
    core, x, y = me % 2, (me // 2) % 2, me // 4
    out = []
    for r in range(4):
        px = 1 - x if r % 2 else x
        py = 1 - y if r // 2 else y
        for p in range(2):
            pc = 1 - core if p else core
            out.append((py * 2 + px) * 2 + pc)
    return out


def _tables(t):
    inv = ROPE_BASE ** (-2.0 * np.arange(HEAD // 2, dtype=np.float64) / HEAD)
    ang = np.arange(t, dtype=np.float64)[:, None] * inv[None, :]
    cos, sin = np.cos(ang), np.sin(ang)
    return (jnp.asarray(np.concatenate([cos, cos], axis=1), F32), jnp.asarray(np.concatenate([-sin, sin], axis=1), F32))


def _dot(a, b):
    return jnp.dot(a, b, preferred_element_type=F32)


def _rms_rows(x, w):
    xf = x.astype(F32)
    r = lax.rsqrt(jnp.mean(xf * xf, axis=-1, keepdims=True) + EPS)
    return (xf * r * w.astype(F32)).astype(BF)


def _dispatch(meta, u, e0, cap, rows, x_ref, gt_ref):
    k = meta.shape[0] // 3
    t = meta.shape[1]
    idx, slot, g = meta[:k], meta[k:2 * k], meta[2 * k:3 * k]
    local = idx - e0
    key = jnp.where((local >= 0.0) & (local < rows // cap), local * cap + slot, -1.0)
    step = 128
    for b in range(rows // step):
        row = lax.broadcasted_iota(jnp.int32, (step, t), 0).astype(F32) + float(b * step)
        d = jnp.zeros((step, t), F32)
        gt = jnp.zeros((step, t), F32)
        for j in range(k):
            hit = row == key[j:j + 1, :]
            d = jnp.where(hit, 1.0, d)
            gt = jnp.where(hit, g[j:j + 1, :], gt)
        col = pl.ds(b * step, step)
        gt = gt.T
        hi = gt.astype(BF)
        rest = gt - hi.astype(F32)
        mid = rest.astype(BF)
        lo = (rest - mid.astype(F32)).astype(BF)
        gt_ref[0:t, col] = hi
        gt_ref[t:2 * t, col] = mid
        gt_ref[2 * t:3 * t, col] = lo
        x_ref[pl.ds(b * step, step), :] = _dot(d.astype(BF), u).astype(BF)


ATT = 8
CH = 4
RING = 3
PASS = (3, 6, 9, 11)
D0 = ATT + 1
E0 = D0 + 8


def _front_kernel(cap, h0_ref, ix_ref, sl_ref, na_ref, nm_ref, cos_ref, sin_ref, wr_ref, wq_ref, wk_ref, wv_ref,
                  wo_ref, ue1_ref, ue3_ref, hid_ref, gt_ref, a_ref,
                  u, meta, acc, kb, vb, xs, ring, own_s, own_r, part_s, part_r, fwd_s, fwd_r, rel_s, rel_r,
                  met_s, met_r, ring_s, hid_s):
    i = pl.program_id(0)
    peers = _peers()
    t, d = h0_ref.shape
    rows = xs.shape[1]
    el = rows // cap
    fe = ue1_ref.shape[2]
    hb = wq_ref.shape[1] // HEAD
    ch = t // CH
    order = (tuple(range(CH)), tuple(range(CH // 2, CH)) + tuple(range(CH // 2)))

    def rc(src, dst, ss, rs, peer):
        return pltpu.make_async_remote_copy(src_ref=src, dst_ref=dst, send_sem=ss, recv_sem=rs,
                                            device_id={'ep': peer}, device_id_type=MESH)

    def own(link, n):
        sl = pl.ds(order[link][n] * ch, ch)
        return rc(u.at[0, sl], u.at[2 + 2 * link, sl], own_s.at[link, n], own_r.at[link, n], peers[2 + 2 * link])

    def part():
        return rc(u.at[0], u.at[1], part_s.at[0], part_r.at[0], peers[1])

    def fwd(link, n):
        sl = pl.ds(order[link][n] * ch, ch)
        return rc(u.at[2 + 2 * link, sl], u.at[3 + 2 * link, sl], fwd_s.at[link, n], fwd_r.at[link, n], peers[1])

    def relay(link, n):
        sl = pl.ds(order[link][n] * ch, ch)
        return rc(u.at[2 + 2 * link, sl], u.at[6, sl], rel_s.at[link, n], rel_r.at[link, n], peers[4 - 2 * link])

    def fwd3(link, n):
        sl = pl.ds(order[link][n] * ch, ch)
        return rc(u.at[6, sl], u.at[7, sl], fwd_s.at[2 + link, n], fwd_r.at[2 + link, n], peers[1])

    def met(s):
        return rc(meta.at[0], meta.at[s], met_s.at[s], met_r.at[s], peers[s])

    def weights(e, j):
        return pltpu.make_async_copy((ue1_ref, ue3_ref)[j].at[e], ring.at[e % RING, j], ring_s.at[e % RING, j])

    def pass_on(n):
        for link in range(2):
            own(link, n).wait_recv()
            if n < CH // 2:
                relay(link, n).start()
            fwd(link, n).start()

    @pl.when(i == 0)
    def _():
        barrier = pltpu.get_barrier_semaphore()
        for s in range(1, 8):
            pl.semaphore_signal(barrier, inc=1, device_id={'ep': peers[s]}, device_id_type=MESH)
        uu = _rms_rows(h0_ref[...], nm_ref[...])
        u[0] = uu
        pl.semaphore_wait(barrier, 7)
        for n in range(CH):
            for link in range(2):
                own(link, n).start()
        part().start()
        for e in range(RING):
            for j in range(2):
                weights(e, j).start()
        xs[7, 0:t] = _rms_rows(h0_ref[...], na_ref[...])
        k = ix_ref.shape[1]
        lt = _dot(uu, wr_ref[...]).T
        it = ix_ref[0]
        ids = lax.broadcasted_iota(jnp.int32, lt.shape, 0)
        sel = [jnp.sum(jnp.where(ids == it[j:j + 1, :], lt, 0.0), axis=0, keepdims=True) for j in range(k)]
        lg = jnp.concatenate(sel, axis=0)
        ex = jnp.exp(lg - jnp.max(lg, axis=0, keepdims=True))
        meta[0, 0:k, :] = it.astype(F32)
        meta[0, k:2 * k, :] = sl_ref[0].astype(F32)
        meta[0, 2 * k:3 * k, :] = ex / jnp.sum(ex, axis=0, keepdims=True)
        acc[...] = h0_ref[...].astype(F32)

    @pl.when(i == 1)
    def _():
        for s in range(1, 8):
            met(s).start()

    for n in range(CH):
        @pl.when(i == PASS[n])
        def _(n=n):
            pass_on(n)

    def rope(v):
        return (v * cos_ref[...] + pltpu.roll(v, HEAD // 2, 1) * sin_ref[...]).astype(BF)

    def project():
        q = _dot(xs[7, 0:t], wq_ref[...])

        def finish():
            for h in range(hb):
                xs[6 + i % 2, t:2 * t, h * HEAD:(h + 1) * HEAD] = rope(q[:, h * HEAD:(h + 1) * HEAD])
        return finish

    def keys():
        g = (i // 2) % 2
        kb[g] = rope(_dot(xs[7, 0:t], wk_ref[...]))
        vb[g] = _dot(xs[7, 0:t], wv_ref[...]).astype(BF)

    def attend(between):
        g = ((i - 1) // 2) % 2
        kk, vv = kb[g], vb[g]
        causal = lax.broadcasted_iota(jnp.int32, (t, t), 0) >= lax.broadcasted_iota(jnp.int32, (t, t), 1)
        sc = [lax.dot_general(xs[6 + (i - 1) % 2, t:2 * t, h * HEAD:(h + 1) * HEAD], kk, (((1,), (1,)), ((), ())),
                              preferred_element_type=F32) for h in range(hb)]
        finish = between()
        o = []
        for h in range(hb):
            s = jnp.where(causal, sc[h] * HEAD ** -0.5, -jnp.inf)
            ex = jnp.exp(s - jnp.max(s, axis=1, keepdims=True))
            p = (ex / jnp.sum(ex, axis=1, keepdims=True)).astype(BF)
            o.append(_dot(p, vv).astype(BF))
        finish()
        acc[...] += _dot(jnp.concatenate(o, axis=1), wo_ref[...])

    @pl.when((i < ATT) & (i % 2 == 0))
    def _():
        keys()

    @pl.when(i == 0)
    def _():
        project()()

    @pl.when((i >= 1) & (i < ATT))
    def _():
        attend(project)

    @pl.when(i == ATT)
    def _():
        attend(lambda: lambda: None)
        a_ref[...] = acc[...].astype(BF)

    for s in range(8):
        @pl.when(i == D0 + s)
        def _(s=s):
            if s == 1:
                part().wait_recv()
            if s in (3, 5):
                for n in range(CH):
                    fwd((s - 3) // 2, n).wait_recv()
            if s == 6:
                for n in range(CH // 2):
                    for link in range(2):
                        relay(link, n).wait_recv()
                        fwd3(link, n).start()
            if s == 7:
                for n in range(CH // 2):
                    for link in range(2):
                        fwd3(link, n).wait_recv()
            if s:
                met(s).wait_recv()
            e0 = lax.axis_index('ep') * el
            _dispatch(meta[s], u[s], e0.astype(F32), cap, rows, xs.at[s], gt_ref.at[0])

    @pl.when(i == E0)
    def _():
        part().wait_send()
        for link in range(2):
            for n in range(CH):
                own(link, n).wait_send()
                fwd(link, n).wait_send()
                if n < CH // 2:
                    relay(link, n).wait_send()
                    fwd3(link, n).wait_send()
        for q in range(1, 8):
            met(q).wait_send()

        def put(n, p):
            return pltpu.make_async_copy(u.at[n, :, pl.ds(p * d // 2, fe)], hid_ref.at[2 * n + p], hid_s.at[n, p])

        @pl.loop(0, el // 2)
        def _(n):
            for p in range(2):
                e = 2 * n + p
                for j in range(2):
                    weights(e, j).wait()
                x = xs[:, pl.ds(pl.multiple_of(e * cap, cap), cap), :].reshape(8 * cap, d)
                h1 = _dot(x, ring[e % RING, 0])
                h3 = _dot(x, ring[e % RING, 1])
                u[n, :, p * d // 2:p * d // 2 + fe] = (h1 * jax.nn.sigmoid(h1) * h3).astype(BF)

                @pl.when(e < el - RING)
                def _():
                    for j in range(2):
                        weights(e + RING, j).start()

                put(n, p).start()

        @pl.loop(0, el // 2)
        def _(n):
            for p in range(2):
                put(n, p).wait()


def _front(h0, idx, slot, na, nm, cos, sin, wr, wq, wk, wv, wo, ue1, ue3, cap):
    t, d = h0.shape
    el, _, fe = ue1.shape
    rows = el * cap
    qb = wq.shape[1] // ATT
    kv = wk.shape[1] // HEAD
    full = lambda a: pl.BlockSpec(a.shape, lambda i: (0,) * a.ndim, pipeline_mode=pl.Buffered(1))
    one = pl.BlockSpec((t, d), lambda i: (0, 0), pipeline_mode=pl.Buffered(1))
    att = lambda i: jnp.minimum(i, ATT - 1)
    prev = lambda i: jnp.clip(i - 1, 0, ATT - 1)
    src = lambda i: jnp.clip(i - D0, 0, 7)
    hbm = pl.BlockSpec(memory_space=pl.ANY)
    dma = pltpu.SemaphoreType.DMA
    return pl.pallas_call(
        lambda *refs: _front_kernel(cap, *refs),
        grid=(E0 + 1,),
        in_specs=[full(h0), full(idx), full(slot), full(na), full(nm), full(cos), full(sin), full(wr),
                  pl.BlockSpec((d, qb), lambda i: (0, att(i))),
                  pl.BlockSpec((d, HEAD), lambda i: (0, att(i) * kv // ATT)),
                  pl.BlockSpec((d, HEAD), lambda i: (0, att(i) * kv // ATT)),
                  pl.BlockSpec((qb, d), lambda i: (prev(i), 0)), hbm, hbm],
        out_specs=[hbm,
                   pl.BlockSpec((1, 3 * t, rows), lambda i: (src(i), 0, 0)), one],
        out_shape=[jax.ShapeDtypeStruct((el, 8 * cap, fe), BF), jax.ShapeDtypeStruct((8, 3 * t, rows), BF),
                   jax.ShapeDtypeStruct((t, d), BF)],
        scratch_shapes=[pltpu.VMEM((8, t, d), BF), pltpu.VMEM((8, 3 * idx.shape[1], t), F32),
                        pltpu.VMEM((t, d), F32),
                        pltpu.VMEM((2, t, HEAD), BF), pltpu.VMEM((2, t, HEAD), BF),
                        pltpu.VMEM((8, rows, d), BF), pltpu.VMEM((RING, 2, d, fe), BF),
                        dma((2, CH)), dma((2, CH)), dma((1,)), dma((1,)), dma((4, CH)), dma((4, CH)),
                        dma((2, CH)), dma((2, CH)), dma((8,)), dma((8,)), dma((RING, 2)), dma((el // 2, 2))],
        compiler_params=pltpu.CompilerParams(dimension_semantics=('arbitrary',), collective_id=0, has_side_effects=True,
                                             vmem_limit_bytes=67043328),
        name='gather_attention_up',
    )(h0, idx, slot, na, nm, cos, sin, wr, wq, wk, wv, wo, ue1, ue3)


NC = 8
FS = 12
LANES = 128
LAG = 2
LATE = 3
POS = ((0, 2, 1, 3), (0, 1, 2, 3))
QE = 2


def _down_kernel(cap, nf_ref, hid_ref, gt_ref, a_ref, ue2_ref, w1_ref, w3_ref, w2_ref, out_ref,
                 hv, gv, ev, w1v, w3v, w2v, hf, yb, mo, mp, r0, r1, r2, acc,
                 h_s, g_s, a_s, e_s, w_s, d_s, d_r, credit, p1_s, p1_r, p2_s, p2_r):
    i = pl.program_id(0)
    peers = _peers()
    el, m, fe = hid_ref.shape
    t, d = a_ref.shape
    nb = d // NC
    fb = w1v.shape[2]
    qe = el // QE

    def rc(src, dst, ss, rs, peer):
        return pltpu.make_async_remote_copy(src_ref=src, dst_ref=dst, send_sem=ss, recv_sem=rs,
                                            device_id={'ep': peer}, device_id_type=MESH)

    def pair(c):
        return rc(mo.at[c % 2], r0.at[c % 2], d_s.at[c % 2], d_r.at[c % 2], peers[1])

    def first(c, b):
        return rc(mp.at[c, b, pl.ds(2, 2)], r1.at[c, b], p1_s.at[c, b], p1_r.at[c, b], peers[2 + 2 * b])

    def second(c, b):
        return rc(mp.at[c, b, 1], r2.at[c, b], p2_s.at[c, b], p2_r.at[c, b], peers[4 - 2 * b])

    def second_step(c):
        for b in range(2):
            first(c, b).wait_recv()
            mp[c, b, pl.ds(0, 2)] = mp[c, b, pl.ds(0, 2)] + r1[c, b]
            second(c, b).start()

    def load_hid(q):
        sl = pl.ds(q * qe, qe)
        return pltpu.make_async_copy(hid_ref.at[sl], hv.at[sl], h_s.at[q])

    def load_gt(q):
        sl = pl.ds(q * 4, 4)
        return pltpu.make_async_copy(gt_ref.at[sl], gv.at[sl], g_s.at[q])

    def load_a():
        return pltpu.make_async_copy(a_ref, out_ref, a_s.at[0])

    def load_down(c, q):
        sl = pl.ds(q * qe, qe)
        return pltpu.make_async_copy(ue2_ref.at[sl, :, pl.ds(pl.multiple_of(c * nb, nb), nb)], ev.at[c % 2, sl],
                                     e_s.at[c % 2, q])

    def load_ffn(n):
        sl = pl.ds(pl.multiple_of(n * fb, fb), fb)
        k = n % 2
        return (pltpu.make_async_copy(w1_ref.at[:, sl], w1v.at[k], w_s.at[k, 0]),
                pltpu.make_async_copy(w3_ref.at[:, sl], w3v.at[k], w_s.at[k, 1]),
                pltpu.make_async_copy(w2_ref.at[sl], w2v.at[k], w_s.at[k, 2]))

    @pl.when(i == 0)
    def _():
        barrier = pltpu.get_barrier_semaphore()
        for s in (1, 2, 4):
            pl.semaphore_signal(barrier, inc=1, device_id={'ep': peers[s]}, device_id_type=MESH)
        for q in range(QE):
            load_hid(q).start()
            load_down(0, q).start()
        for q in range(2):
            load_gt(q).start()
        load_a().start()
        for cp in load_ffn(0):
            cp.start()
        for q in range(QE):
            load_hid(q).wait()
        pl.semaphore_wait(barrier, 3)

    @pl.when(i + 1 < NC)
    def _():
        for q in range(QE):
            load_down(i + 1, q).start()

    @pl.when(i + 1 < FS)
    def _():
        for cp in load_ffn(i + 1):
            cp.start()

    @pl.when((i >= LAG) & (i < NC))
    def _():
        second_step(i - LAG)

    for c in range(NC - LAG, NC):
        @pl.when(i == NC + LATE * (c - NC + LAG))
        def _(c=c):
            second_step(c)

    @pl.when(i < NC)
    def _():
        for q in range(QE):
            load_down(i, q).wait()
            for e in range(q * qe, (q + 1) * qe):
                y = _dot(hv[e], ev[i % 2, e]).astype(BF)
                for s in range(8):
                    yb[s, e * cap:(e + 1) * cap, :] = y[s * cap:(s + 1) * cap]

    @pl.when(i == 0)
    def _():
        for q in range(2):
            load_gt(q).wait()

    @pl.when((i >= 2) & (i < NC))
    def _():
        pl.semaphore_wait(credit, 1)

    def combine(s):
        v = _dot(gv[s], yb[s])
        v = v[:t] + v[t:2 * t] + v[2 * t:]
        for b in range(2):
            dst = v[:, b * LANES:(b + 1) * LANES]
            if s % 2:
                mo[i % 2, b, POS[b][s // 2]] = dst
            else:
                mp[i, b, POS[b][s // 2]] = dst

    @pl.when(i < NC)
    def _():
        for s in range(1, 8, 2):
            combine(s)
        pair(i).start()
        for s in range(0, 8, 2):
            combine(s)

    @pl.when(i == 0)
    def _():
        load_a().wait()
        acc[...] = out_ref[...].astype(F32)
        out_ref[...] = _rms_rows(out_ref[...], nf_ref[...])

    for cp in load_ffn(i):
        cp.wait()
    h1 = _dot(out_ref[...], w1v[i % 2])
    h3 = _dot(out_ref[...], w3v[i % 2])
    hf[...] = (h1 * jax.nn.sigmoid(h1) * h3).astype(BF)

    @pl.when(i < NC)
    def _():
        pair(i).wait()
        mp[i] = mp[i] + r0[i % 2]

        @pl.when(i < NC - 2)
        def _():
            pl.semaphore_signal(credit, inc=1, device_id={'ep': peers[1]}, device_id_type=MESH)

        for b in range(2):
            first(i, b).start()

    acc[...] += _dot(hf[...], w2v[i % 2])

    @pl.when(i == FS - 1)
    def _():
        for c in range(NC):
            for b in range(2):
                second(c, b).wait_recv()
                col = pl.ds((2 * c + b) * LANES, LANES)
                out_ref[:, col] = (acc[:, col] + (mp[c, b, 0] + r2[c, b])).astype(BF)
        for c in range(NC):
            for b in range(2):
                first(c, b).wait_send()
                second(c, b).wait_send()


def _down(hid, gt, a, nf, ue2, w1, w3, w2, cap):
    el, m, fe = hid.shape
    t, d = a.shape
    nb = d // NC
    fb = w1.shape[1] // FS
    hbm = pl.BlockSpec(memory_space=pl.ANY)
    dma = pltpu.SemaphoreType.DMA
    return pl.pallas_call(
        lambda *refs: _down_kernel(cap, *refs),
        grid=(FS,),
        in_specs=[pl.BlockSpec(nf.shape, lambda i: (0,), pipeline_mode=pl.Buffered(1))] + [hbm] * 7,
        out_specs=pl.BlockSpec((t, d), lambda i: (0, 0), pipeline_mode=pl.Buffered(1)),
        out_shape=jax.ShapeDtypeStruct((t, d), BF),
        scratch_shapes=[pltpu.VMEM(hid.shape, BF), pltpu.VMEM(gt.shape, BF),
                        pltpu.VMEM((2, el, fe, nb), BF), pltpu.VMEM((2, d, fb), BF), pltpu.VMEM((2, d, fb), BF),
                        pltpu.VMEM((2, fb, d), BF), pltpu.VMEM((t, fb), BF),
                        pltpu.VMEM((8, el * cap, nb), BF),
                        pltpu.VMEM((2, 2, 4, t, LANES), F32), pltpu.VMEM((NC, 2, 4, t, LANES), F32),
                        pltpu.VMEM((2, 2, 4, t, LANES), F32), pltpu.VMEM((NC, 2, 2, t, LANES), F32),
                        pltpu.VMEM((NC, 2, t, LANES), F32), pltpu.VMEM((t, d), F32),
                        dma((QE,)), dma((2,)), dma((1,)), dma((2, QE)), dma((2, 3)),
                        dma((2,)), dma((2,)), pltpu.SemaphoreType.REGULAR,
                        dma((NC, 2)), dma((NC, 2)), dma((NC, 2)), dma((NC, 2))],
        compiler_params=pltpu.CompilerParams(dimension_semantics=('arbitrary',), collective_id=1, has_side_effects=True,
                                             vmem_limit_bytes=67043328),
        name='expert_down_ffn',
    )(nf, hid, gt, a, ue2, w1, w3, w2)


def solution(mesh):
    G = mesh.shape['ep']

    def local(h0, idx, slot, na, wq, wk, wv, wo, nf, w1, w3, w2, nm, wr, ue1, ue3, ue2):
        b, s, d = h0.shape
        k = idx.shape[-1]
        el = ue1.shape[0]
        cap = 2 * s * k // (el * G)
        cos, sin = _tables(s)
        h = h0.reshape(s, d)
        hid, gt, a = _front(h, jnp.swapaxes(idx, 1, 2), jnp.swapaxes(slot, 1, 2), na, nm, cos, sin, wr, wq, wk, wv,
                               wo, ue1, ue3, cap)
        return _down(hid, gt, a, nf, ue2, w1, w3, w2, cap).reshape(b, s, d)

    rows_spec = P(('dp', 'ep'))
    in_specs = (rows_spec,) * 3 + (P(),) * 11 + (P('ep'),) * 3
    return jax.shard_map(local, mesh=mesh, in_specs=in_specs, out_specs=rows_spec, check_vma=False)
```

```python
import jax
import jax.numpy as jnp
import numpy as np
from jax import lax
from jax.experimental import pallas as pl
from jax.experimental.pallas import tpu as pltpu
from jax.sharding import PartitionSpec as P

HEAD = 128
EPS = 1e-6
ROPE_BASE = 10000.0
MESH = pl.DeviceIdType.MESH
F32 = jnp.float32
BF = jnp.bfloat16
VMEM_LIMIT = 62 * 1024 * 1024


def _peers():
    me = lax.axis_index('ep')
    core, x, y = me % 2, (me // 2) % 2, me // 4
    out = []
    for r in range(4):
        px = 1 - x if r % 2 else x
        py = 1 - y if r // 2 else y
        for p in range(2):
            pc = 1 - core if p else core
            out.append((py * 2 + px) * 2 + pc)
    return out


def _tables(t):
    inv = ROPE_BASE ** (-2.0 * np.arange(HEAD // 2, dtype=np.float64) / HEAD)
    ang = np.arange(t, dtype=np.float64)[:, None] * inv[None, :]
    cos, sin = np.cos(ang), np.sin(ang)
    return (jnp.asarray(np.concatenate([cos, cos], axis=1), F32), jnp.asarray(np.concatenate([-sin, sin], axis=1), F32))


def _dot(a, b):
    return jnp.dot(a, b, preferred_element_type=F32)


def _rms_rows(x, w):
    xf = x.astype(F32)
    r = lax.rsqrt(jnp.mean(xf * xf, axis=-1, keepdims=True) + EPS)
    return (xf * r * w.astype(F32)).astype(BF)


def _places(meta, e0, cap, rows, d_ref, gt_ref):
    k = meta.shape[0] // 3
    t = meta.shape[1]
    idx, slot, g = meta[:k], meta[k:2 * k], meta[2 * k:3 * k]
    local = idx - e0
    key = jnp.where((local >= 0.0) & (local < rows // cap), local * cap + slot, -1.0)
    step = 128
    for b in range(rows // step):
        row = lax.broadcasted_iota(jnp.int32, (step, t), 0).astype(F32) + float(b * step)
        d = jnp.zeros((step, t), F32)
        gt = jnp.zeros((step, t), F32)
        for j in range(k):
            hit = row == key[j:j + 1, :]
            d = jnp.where(hit, 1.0, d)
            gt = jnp.where(hit, g[j:j + 1, :], gt)
        col = pl.ds(b * step, step)
        d_ref[col, :] = d.astype(BF)
        gt = gt.T
        hi = gt.astype(BF)
        rest = gt - hi.astype(F32)
        mid = rest.astype(BF)
        lo = (rest - mid.astype(F32)).astype(BF)
        gt_ref[0:t, col] = hi
        gt_ref[t:2 * t, col] = mid
        gt_ref[2 * t:3 * t, col] = lo


ATT = 8
CH = 4
RING = 3
PASS = (3, 6, 9, 11)
D0 = ATT + 1
E0 = D0 + 8


def _front_kernel(cap, h0_ref, ix_ref, sl_ref, na_ref, nm_ref, cos_ref, sin_ref, wr_ref, wq_ref, wk_ref, wv_ref,
                  wo_ref, ue1_ref, ue3_ref, hid_ref, gt_ref, a_ref,
                  u, meta, acc, kb, vb, xs, ring, db, wqv, wkv, wvv, wov, wrv, own_s, own_r, part_s, part_r, fwd_s, fwd_r, rel_s, rel_r,
                  met_s, met_r, ring_s, hid_s, q_s, kv_s, o_s, wr_s):
    i = pl.program_id(0)
    peers = _peers()
    t, d = h0_ref.shape
    rows = xs.shape[1]
    el = rows // cap
    fe = ue1_ref.shape[2]
    qw = wqv.shape[2]
    hb = qw // HEAD
    ch = t // CH
    order = (tuple(range(CH)), tuple(range(CH // 2, CH)) + tuple(range(CH // 2)))

    def rc(src, dst, ss, rs, peer):
        return pltpu.make_async_remote_copy(src_ref=src, dst_ref=dst, send_sem=ss, recv_sem=rs,
                                            device_id={'ep': peer}, device_id_type=MESH)

    def own(link, n):
        sl = pl.ds(order[link][n] * ch, ch)
        return rc(u.at[0, sl], u.at[2 + 2 * link, sl], own_s.at[link, n], own_r.at[link, n], peers[2 + 2 * link])

    def part():
        return rc(u.at[0], u.at[1], part_s.at[0], part_r.at[0], peers[1])

    def fwd(link, n):
        sl = pl.ds(order[link][n] * ch, ch)
        return rc(u.at[2 + 2 * link, sl], u.at[3 + 2 * link, sl], fwd_s.at[link, n], fwd_r.at[link, n], peers[1])

    def relay(link, n):
        sl = pl.ds(order[link][n] * ch, ch)
        return rc(u.at[2 + 2 * link, sl], u.at[6, sl], rel_s.at[link, n], rel_r.at[link, n], peers[4 - 2 * link])

    def fwd3(link, n):
        sl = pl.ds(order[link][n] * ch, ch)
        return rc(u.at[6, sl], u.at[7, sl], fwd_s.at[2 + link, n], fwd_r.at[2 + link, n], peers[1])

    def met(s):
        return rc(meta.at[0], meta.at[s], met_s.at[s], met_r.at[s], peers[s])

    def weights(e, j):
        return pltpu.make_async_copy((ue1_ref, ue3_ref)[j].at[e], ring.at[e % RING, j], ring_s.at[e % RING, j])

    def load_q(n):
        sl = pl.ds(pl.multiple_of(n * qw, qw), qw)
        return pltpu.make_async_copy(wq_ref.at[:, sl], wqv.at[n % 2], q_s.at[n % 2])

    def load_o(n):
        sl = pl.ds(pl.multiple_of(n * qw, qw), qw)
        return pltpu.make_async_copy(wo_ref.at[sl], wov.at[n % 2], o_s.at[n % 2])

    def load_kv(g, j):
        sl = pl.ds(pl.multiple_of(g * HEAD, HEAD), HEAD)
        return pltpu.make_async_copy((wk_ref, wv_ref)[j].at[:, sl], (wkv, wvv)[j].at[g % 2], kv_s.at[g % 2, j])

    def load_r():
        return pltpu.make_async_copy(wr_ref, wrv, wr_s.at[0])

    def pass_on(n):
        for link in range(2):
            own(link, n).wait_recv()
            if n < CH // 2:
                relay(link, n).start()
            fwd(link, n).start()

    @pl.when(i == 0)
    def _():
        barrier = pltpu.get_barrier_semaphore()
        for s in range(1, 8):
            pl.semaphore_signal(barrier, inc=1, device_id={'ep': peers[s]}, device_id_type=MESH)
        uu = _rms_rows(h0_ref[...], nm_ref[...])
        u[0] = uu
        pl.semaphore_wait(barrier, 7)
        for n in range(CH):
            for link in range(2):
                own(link, n).start()
        part().start()
        load_r().start()
        load_q(0).start()
        for j in range(2):
            load_kv(0, j).start()
        xs[7, 0:t] = _rms_rows(h0_ref[...], na_ref[...])
        k = ix_ref.shape[1]
        load_r().wait()
        lt = _dot(uu, wrv[...]).T
        it = ix_ref[0]
        ids = lax.broadcasted_iota(jnp.int32, lt.shape, 0)
        sel = [jnp.sum(jnp.where(ids == it[j:j + 1, :], lt, 0.0), axis=0, keepdims=True) for j in range(k)]
        lg = jnp.concatenate(sel, axis=0)
        ex = jnp.exp(lg - jnp.max(lg, axis=0, keepdims=True))
        meta[0, 0:k, :] = it.astype(F32)
        meta[0, k:2 * k, :] = sl_ref[0].astype(F32)
        meta[0, 2 * k:3 * k, :] = ex / jnp.sum(ex, axis=0, keepdims=True)
        acc[...] = h0_ref[...].astype(F32)

    @pl.when(i == 1)
    def _():
        for s in range(1, 8):
            met(s).start()

    @pl.when(i == ATT // 2)
    def _():
        for e in range(RING):
            for j in range(2):
                weights(e, j).start()

    @pl.when(i + 1 < ATT)
    def _():
        load_q(i + 1).start()

    @pl.when(i < ATT)
    def _():
        load_o(i).start()

    @pl.when((i % 2 == 1) & (i + 1 < ATT))
    def _():
        for j in range(2):
            load_kv((i + 1) // 2, j).start()

    for n in range(CH):
        @pl.when(i == PASS[n])
        def _(n=n):
            pass_on(n)

    def rope(v):
        return (v * cos_ref[...] + pltpu.roll(v, HEAD // 2, 1) * sin_ref[...]).astype(BF)

    def project():
        q = _dot(xs[7, 0:t], wqv[i % 2])

        def finish():
            for h in range(hb):
                xs[6 + i % 2, t:2 * t, h * HEAD:(h + 1) * HEAD] = rope(q[:, h * HEAD:(h + 1) * HEAD])
        return finish

    def keys():
        g = (i // 2) % 2
        for j in range(2):
            load_kv(i // 2, j).wait()
        kb[g] = rope(_dot(xs[7, 0:t], wkv[g]))
        vb[g] = _dot(xs[7, 0:t], wvv[g]).astype(BF)

    def attend(between):
        g = ((i - 1) // 2) % 2
        kk, vv = kb[g], vb[g]
        causal = lax.broadcasted_iota(jnp.int32, (t, t), 0) >= lax.broadcasted_iota(jnp.int32, (t, t), 1)
        sc = [lax.dot_general(xs[6 + (i - 1) % 2, t:2 * t, h * HEAD:(h + 1) * HEAD], kk, (((1,), (1,)), ((), ())),
                              preferred_element_type=F32) for h in range(hb)]
        finish = between()
        o = []
        for h in range(hb):
            s = jnp.where(causal, sc[h] * HEAD ** -0.5, -jnp.inf)
            ex = jnp.exp(s - jnp.max(s, axis=1, keepdims=True))
            p = (ex / jnp.sum(ex, axis=1, keepdims=True)).astype(BF)
            o.append(_dot(p, vv).astype(BF))
        finish()
        acc[...] += _dot(jnp.concatenate(o, axis=1), wov[(i - 1) % 2])

    @pl.when((i < ATT) & (i % 2 == 0))
    def _():
        keys()

    @pl.when(i < ATT)
    def _():
        load_q(i).wait()

    @pl.when((i >= 1) & (i <= ATT))
    def _():
        load_o(i - 1).wait()

    @pl.when(i == 0)
    def _():
        project()()

    @pl.when((i >= 1) & (i < ATT))
    def _():
        attend(project)

    @pl.when(i == ATT)
    def _():
        attend(lambda: lambda: None)
        a_ref[...] = acc[...].astype(BF)

    for s in range(8):
        @pl.when(i == D0 + s)
        def _(s=s):
            if s:
                met(s).wait_recv()
            e0 = lax.axis_index('ep') * el
            _places(meta[s], e0.astype(F32), cap, rows, db, gt_ref.at[0])
            if s == 1:
                part().wait_recv()
            if s in (3, 5):
                for n in range(CH):
                    fwd((s - 3) // 2, n).wait_recv()
            if s == 6:
                for n in range(CH // 2):
                    for link in range(2):
                        relay(link, n).wait_recv()
                        fwd3(link, n).start()
            if s == 7:
                for n in range(CH // 2):
                    for link in range(2):
                        fwd3(link, n).wait_recv()
            xs[s] = _dot(db[...], u[s]).astype(BF)

    @pl.when(i == E0)
    def _():
        part().wait_send()
        for link in range(2):
            for n in range(CH):
                own(link, n).wait_send()
                fwd(link, n).wait_send()
                if n < CH // 2:
                    relay(link, n).wait_send()
                    fwd3(link, n).wait_send()
        for q in range(1, 8):
            met(q).wait_send()

        def put(n, p):
            return pltpu.make_async_copy(u.at[n, :, pl.ds(p * d // 2, fe)], hid_ref.at[2 * n + p], hid_s.at[n, p])

        @pl.loop(0, el // 2)
        def _(n):
            for p in range(2):
                e = 2 * n + p
                for j in range(2):
                    weights(e, j).wait()
                x = xs[:, pl.ds(pl.multiple_of(e * cap, cap), cap), :].reshape(8 * cap, d)
                h1 = _dot(x, ring[e % RING, 0])
                h3 = _dot(x, ring[e % RING, 1])
                u[n, :, p * d // 2:p * d // 2 + fe] = (h1 * jax.nn.sigmoid(h1) * h3).astype(BF)

                @pl.when(e < el - RING)
                def _():
                    for j in range(2):
                        weights(e + RING, j).start()

                put(n, p).start()

        @pl.loop(0, el // 2)
        def _(n):
            for p in range(2):
                put(n, p).wait()


def _front(h0, idx, slot, na, nm, cos, sin, wr, wq, wk, wv, wo, ue1, ue3, cap):
    t, d = h0.shape
    el, _, fe = ue1.shape
    rows = el * cap
    qb = wq.shape[1] // ATT
    full = lambda a: pl.BlockSpec(a.shape, lambda i: (0,) * a.ndim, pipeline_mode=pl.Buffered(1))
    one = pl.BlockSpec((t, d), lambda i: (0, 0), pipeline_mode=pl.Buffered(1))

    def src(i):
        s = jnp.clip(i - D0, 0, 7)
        return s // 2 + 4 * (1 - s % 2)

    hbm = pl.BlockSpec(memory_space=pl.ANY)
    dma = pltpu.SemaphoreType.DMA
    return pl.pallas_call(
        lambda *refs: _front_kernel(cap, *refs),
        grid=(E0 + 1,),
        in_specs=[full(h0), full(idx), full(slot), full(na), full(nm), full(cos), full(sin)] + [hbm] * 7,
        out_specs=[hbm,
                   pl.BlockSpec((1, 3 * t, rows), lambda i: (src(i), 0, 0)), one],
        out_shape=[jax.ShapeDtypeStruct((el, 8 * cap, fe), BF), jax.ShapeDtypeStruct((8, 3 * t, rows), BF),
                   jax.ShapeDtypeStruct((t, d), BF)],
        scratch_shapes=[pltpu.VMEM((8, t, d), BF), pltpu.VMEM((8, 3 * idx.shape[1], t), F32),
                        pltpu.VMEM((t, d), F32),
                        pltpu.VMEM((2, t, HEAD), BF), pltpu.VMEM((2, t, HEAD), BF),
                        pltpu.VMEM((8, rows, d), BF), pltpu.VMEM((RING, 2, d, fe), BF),
                        pltpu.VMEM((rows, t), BF), pltpu.VMEM((2, d, qb), BF), pltpu.VMEM((2, d, HEAD), BF),
                        pltpu.VMEM((2, d, HEAD), BF), pltpu.VMEM((2, qb, d), BF), pltpu.VMEM(wr.shape, BF),
                        dma((2, CH)), dma((2, CH)), dma((1,)), dma((1,)), dma((4, CH)), dma((4, CH)),
                        dma((2, CH)), dma((2, CH)), dma((8,)), dma((8,)), dma((RING, 2)), dma((el // 2, 2)),
                        dma((2,)), dma((2, 2)), dma((2,)), dma((1,))],
        compiler_params=pltpu.CompilerParams(dimension_semantics=('arbitrary',), collective_id=0, has_side_effects=True,
                                             vmem_limit_bytes=67043328),
        name='gather_attention_up',
    )(h0, idx, slot, na, nm, cos, sin, wr, wq, wk, wv, wo, ue1, ue3)


NC = 8
FS = 12
LANES = 128
LAG = 2
LATE = 3
POS = ((0, 2, 1, 3), (0, 1, 2, 3))
QE = 2


def _down_kernel(cap, nf_ref, hid_ref, gt_ref, a_ref, ue2_ref, w1_ref, w3_ref, w2_ref, out_ref,
                 hv, gv, ev, w1v, w3v, w2v, hf, yb, mo, mp, r0, r1, r2, acc,
                 h_s, g_s, a_s, e_s, w_s, d_s, d_r, credit, p1_s, p1_r, p2_s, p2_r):
    i = pl.program_id(0)
    peers = _peers()
    el, m, fe = hid_ref.shape
    t, d = a_ref.shape
    nb = d // NC
    fb = w1v.shape[2]
    qe = el // QE

    def rc(src, dst, ss, rs, peer):
        return pltpu.make_async_remote_copy(src_ref=src, dst_ref=dst, send_sem=ss, recv_sem=rs,
                                            device_id={'ep': peer}, device_id_type=MESH)

    def pair(c):
        return rc(mo.at[c % 2], r0.at[c % 2], d_s.at[c % 2], d_r.at[c % 2], peers[1])

    def first(c, b):
        return rc(mp.at[c, b, pl.ds(2, 2)], r1.at[c, b], p1_s.at[c, b], p1_r.at[c, b], peers[2 + 2 * b])

    def second(c, b):
        return rc(mp.at[c, b, 1], r2.at[c, b], p2_s.at[c, b], p2_r.at[c, b], peers[4 - 2 * b])

    def second_step(c):
        for b in range(2):
            first(c, b).wait_recv()
            mp[c, b, pl.ds(0, 2)] = mp[c, b, pl.ds(0, 2)] + r1[c, b]
            second(c, b).start()

    def load_hid(q):
        sl = pl.ds(q * qe, qe)
        return pltpu.make_async_copy(hid_ref.at[sl], hv.at[sl], h_s.at[q])

    def load_gt(q):
        sl = pl.ds(q * 4, 4)
        return pltpu.make_async_copy(gt_ref.at[sl], gv.at[sl], g_s.at[q])

    def load_a():
        return pltpu.make_async_copy(a_ref, out_ref, a_s.at[0])

    def load_down(c, q):
        sl = pl.ds(q * qe, qe)
        return pltpu.make_async_copy(ue2_ref.at[sl, :, pl.ds(pl.multiple_of(c * nb, nb), nb)], ev.at[c % 2, sl],
                                     e_s.at[c % 2, q])

    def load_ffn(n):
        sl = pl.ds(pl.multiple_of(n * fb, fb), fb)
        k = n % 2
        return (pltpu.make_async_copy(w1_ref.at[:, sl], w1v.at[k], w_s.at[k, 0]),
                pltpu.make_async_copy(w3_ref.at[:, sl], w3v.at[k], w_s.at[k, 1]),
                pltpu.make_async_copy(w2_ref.at[sl], w2v.at[k], w_s.at[k, 2]))

    @pl.when(i == 0)
    def _():
        barrier = pltpu.get_barrier_semaphore()
        for s in (1, 2, 4):
            pl.semaphore_signal(barrier, inc=1, device_id={'ep': peers[s]}, device_id_type=MESH)
        for q in range(QE):
            load_hid(q).start()
            load_down(0, q).start()
        for q in range(2):
            load_gt(q).start()
        load_a().start()
        pl.semaphore_wait(barrier, 3)

    def prefetch():
        @pl.when(i + 1 < NC)
        def _():
            for q in range(QE):
                load_down(i + 1, q).start()

        @pl.when(i + 1 < FS)
        def _():
            for cp in load_ffn(i + 1):
                cp.start()

    @pl.when(i > 0)
    def _():
        prefetch()

    @pl.when((i >= LAG) & (i < NC))
    def _():
        second_step(i - LAG)

    for c in range(NC - LAG, NC):
        @pl.when(i == NC + LATE * (c - NC + LAG))
        def _(c=c):
            second_step(c)

    @pl.when(i < NC)
    def _():
        for q in range(QE):
            @pl.when(i == 0)
            def _(q=q):
                load_hid(q).wait()

            load_down(i, q).wait()
            for e in range(q * qe, (q + 1) * qe):
                y = _dot(hv[e], ev[i % 2, e]).astype(BF)
                for s in range(8):
                    yb[s, e * cap:(e + 1) * cap, :] = y[s * cap:(s + 1) * cap]

    @pl.when(i == 0)
    def _():
        load_gt(0).wait()
        for cp in load_ffn(0):
            cp.start()
        prefetch()

    @pl.when((i >= 2) & (i < NC))
    def _():
        pl.semaphore_wait(credit, 1)

    def combine(s):
        v = _dot(gv[s // 2 + 4 * (1 - s % 2)], yb[s])
        v = v[:t] + v[t:2 * t] + v[2 * t:]
        for b in range(2):
            dst = v[:, b * LANES:(b + 1) * LANES]
            if s % 2:
                mo[i % 2, b, POS[b][s // 2]] = dst
            else:
                mp[i, b, POS[b][s // 2]] = dst

    @pl.when(i < NC)
    def _():
        for s in range(1, 8, 2):
            combine(s)
        pair(i).start()

        @pl.when(i == 0)
        def _():
            load_gt(1).wait()

        for s in range(0, 8, 2):
            combine(s)

    @pl.when(i == 0)
    def _():
        load_a().wait()
        acc[...] = out_ref[...].astype(F32)
        out_ref[...] = _rms_rows(out_ref[...], nf_ref[...])

    for cp in load_ffn(i):
        cp.wait()
    h1 = _dot(out_ref[...], w1v[i % 2])
    h3 = _dot(out_ref[...], w3v[i % 2])
    hf[...] = (h1 * jax.nn.sigmoid(h1) * h3).astype(BF)

    @pl.when(i < NC)
    def _():
        pair(i).wait()
        mp[i] = mp[i] + r0[i % 2]

        @pl.when(i < NC - 2)
        def _():
            pl.semaphore_signal(credit, inc=1, device_id={'ep': peers[1]}, device_id_type=MESH)

        for b in range(2):
            first(i, b).start()

    acc[...] += _dot(hf[...], w2v[i % 2])

    @pl.when(i == FS - 1)
    def _():
        for c in range(NC):
            for b in range(2):
                second(c, b).wait_recv()
                col = pl.ds((2 * c + b) * LANES, LANES)
                out_ref[:, col] = (acc[:, col] + (mp[c, b, 0] + r2[c, b])).astype(BF)
        for c in range(NC):
            for b in range(2):
                first(c, b).wait_send()
                second(c, b).wait_send()


def _down(hid, gt, a, nf, ue2, w1, w3, w2, cap):
    el, m, fe = hid.shape
    t, d = a.shape
    nb = d // NC
    fb = w1.shape[1] // FS
    hbm = pl.BlockSpec(memory_space=pl.ANY)
    dma = pltpu.SemaphoreType.DMA
    return pl.pallas_call(
        lambda *refs: _down_kernel(cap, *refs),
        grid=(FS,),
        in_specs=[pl.BlockSpec(nf.shape, lambda i: (0,), pipeline_mode=pl.Buffered(1))] + [hbm] * 7,
        out_specs=pl.BlockSpec((t, d), lambda i: (0, 0), pipeline_mode=pl.Buffered(1)),
        out_shape=jax.ShapeDtypeStruct((t, d), BF),
        scratch_shapes=[pltpu.VMEM(hid.shape, BF), pltpu.VMEM(gt.shape, BF),
                        pltpu.VMEM((2, el, fe, nb), BF), pltpu.VMEM((2, d, fb), BF), pltpu.VMEM((2, d, fb), BF),
                        pltpu.VMEM((2, fb, d), BF), pltpu.VMEM((t, fb), BF),
                        pltpu.VMEM((8, el * cap, nb), BF),
                        pltpu.VMEM((2, 2, 4, t, LANES), F32), pltpu.VMEM((NC, 2, 4, t, LANES), F32),
                        pltpu.VMEM((2, 2, 4, t, LANES), F32), pltpu.VMEM((NC, 2, 2, t, LANES), F32),
                        pltpu.VMEM((NC, 2, t, LANES), F32), pltpu.VMEM((t, d), F32),
                        dma((QE,)), dma((2,)), dma((1,)), dma((2, QE)), dma((2, 3)),
                        dma((2,)), dma((2,)), pltpu.SemaphoreType.REGULAR,
                        dma((NC, 2)), dma((NC, 2)), dma((NC, 2)), dma((NC, 2))],
        compiler_params=pltpu.CompilerParams(dimension_semantics=('arbitrary',), collective_id=1, has_side_effects=True,
                                             vmem_limit_bytes=67043328),
        name='expert_down_ffn',
    )(nf, hid, gt, a, ue2, w1, w3, w2)


def solution(mesh):
    G = mesh.shape['ep']

    def local(h0, idx, slot, na, wq, wk, wv, wo, nf, w1, w3, w2, nm, wr, ue1, ue3, ue2):
        b, s, d = h0.shape
        k = idx.shape[-1]
        el = ue1.shape[0]
        cap = 2 * s * k // (el * G)
        cos, sin = _tables(s)
        h = h0.reshape(s, d)
        hid, gt, a = _front(h, jnp.swapaxes(idx, 1, 2), jnp.swapaxes(slot, 1, 2), na, nm, cos, sin, wr, wq, wk, wv,
                               wo, ue1, ue3, cap)
        return _down(hid, gt, a, nf, ue2, w1, w3, w2, cap).reshape(b, s, d)

    rows_spec = P(('dp', 'ep'))
    in_specs = (rows_spec,) * 3 + (P(),) * 11 + (P('ep'),) * 3
    return jax.shard_map(local, mesh=mesh, in_specs=in_specs, out_specs=rows_spec, check_vma=False)
```

```python
import jax
import jax.numpy as jnp
import numpy as np
from jax import lax
from jax.experimental import pallas as pl
from jax.experimental.pallas import tpu as pltpu
from jax.sharding import PartitionSpec as P

HEAD = 128
EPS = 1e-6
ROPE_BASE = 10000.0
MESH = pl.DeviceIdType.MESH
F32 = jnp.float32
BF = jnp.bfloat16
VMEM_LIMIT = 62 * 1024 * 1024


def _peers():
    me = lax.axis_index('ep')
    core, x, y = me % 2, (me // 2) % 2, me // 4
    out = []
    for r in range(4):
        px = 1 - x if r % 2 else x
        py = 1 - y if r // 2 else y
        for p in range(2):
            pc = 1 - core if p else core
            out.append((py * 2 + px) * 2 + pc)
    return out


def _tables(t):
    inv = ROPE_BASE ** (-2.0 * np.arange(HEAD // 2, dtype=np.float64) / HEAD)
    ang = np.arange(t, dtype=np.float64)[:, None] * inv[None, :]
    cos, sin = np.cos(ang), np.sin(ang)
    return (jnp.asarray(np.concatenate([cos, cos], axis=1), F32), jnp.asarray(np.concatenate([-sin, sin], axis=1), F32))


def _dot(a, b):
    return jnp.dot(a, b, preferred_element_type=F32)


def _rms_rows(x, w):
    xf = x.astype(F32)
    r = lax.rsqrt(jnp.mean(xf * xf, axis=-1, keepdims=True) + EPS)
    return (xf * r * w.astype(F32)).astype(BF)


def _places(meta, e0, cap, rows, d_ref, gt_ref):
    k = meta.shape[0] // 3
    t = meta.shape[1]
    idx, slot, g = meta[:k], meta[k:2 * k], meta[2 * k:3 * k]
    local = idx - e0
    key = jnp.where((local >= 0.0) & (local < rows // cap), local * cap + slot, -1.0)
    step = 128
    for b in range(rows // step):
        row = lax.broadcasted_iota(jnp.int32, (step, t), 0).astype(F32) + float(b * step)
        d = jnp.zeros((step, t), F32)
        gt = jnp.zeros((step, t), F32)
        for j in range(k):
            hit = row == key[j:j + 1, :]
            d = jnp.where(hit, 1.0, d)
            gt = jnp.where(hit, g[j:j + 1, :], gt)
        col = pl.ds(b * step, step)
        d_ref[col, :] = d.astype(BF)
        gt = gt.T
        hi = gt.astype(BF)
        rest = gt - hi.astype(F32)
        mid = rest.astype(BF)
        lo = (rest - mid.astype(F32)).astype(BF)
        gt_ref[0:t, col] = hi
        gt_ref[t:2 * t, col] = mid
        gt_ref[2 * t:3 * t, col] = lo


ATT = 8
CH = 4
RING = 3
PASS = (3, 6, 9, 11)
D0 = ATT + 1
E0 = D0 + 8


def _front_kernel(cap, h0_ref, ix_ref, sl_ref, na_ref, nm_ref, cos_ref, sin_ref, wr_ref, wq_ref, wk_ref, wv_ref,
                  wo_ref, ue1_ref, ue3_ref, hid_ref, gt_ref, a_ref,
                  u, meta, acc, kb, vb, xs, ring, db, wqv, wkv, wvv, wov, wrv, own_s, own_r, part_s, part_r, fwd_s, fwd_r, rel_s, rel_r,
                  met_s, met_r, ring_s, hid_s, q_s, kv_s, o_s, wr_s):
    i = pl.program_id(0)
    peers = _peers()
    t, d = h0_ref.shape
    rows = xs.shape[1]
    el = rows // cap
    fe = ue1_ref.shape[2]
    qw = wqv.shape[2]
    hb = qw // HEAD
    ch = t // CH
    order = (tuple(range(CH)), tuple(range(CH // 2, CH)) + tuple(range(CH // 2)))

    def rc(src, dst, ss, rs, peer):
        return pltpu.make_async_remote_copy(src_ref=src, dst_ref=dst, send_sem=ss, recv_sem=rs,
                                            device_id={'ep': peer}, device_id_type=MESH)

    def own(link, n):
        sl = pl.ds(order[link][n] * ch, ch)
        return rc(u.at[0, sl], u.at[2 + 2 * link, sl], own_s.at[link, n], own_r.at[link, n], peers[2 + 2 * link])

    def part():
        return rc(u.at[0], u.at[1], part_s.at[0], part_r.at[0], peers[1])

    def fwd(link, n):
        sl = pl.ds(order[link][n] * ch, ch)
        return rc(u.at[2 + 2 * link, sl], u.at[3 + 2 * link, sl], fwd_s.at[link, n], fwd_r.at[link, n], peers[1])

    def relay(link, n):
        sl = pl.ds(order[link][n] * ch, ch)
        return rc(u.at[2 + 2 * link, sl], u.at[6, sl], rel_s.at[link, n], rel_r.at[link, n], peers[4 - 2 * link])

    def fwd3(link, n):
        sl = pl.ds(order[link][n] * ch, ch)
        return rc(u.at[6, sl], u.at[7, sl], fwd_s.at[2 + link, n], fwd_r.at[2 + link, n], peers[1])

    def met(s):
        return rc(meta.at[0], meta.at[s], met_s.at[s], met_r.at[s], peers[s])

    def weights(e, j):
        return pltpu.make_async_copy((ue1_ref, ue3_ref)[j].at[e], ring.at[e % RING, j], ring_s.at[e % RING, j])

    def load_q(n):
        sl = pl.ds(pl.multiple_of(n * qw, qw), qw)
        return pltpu.make_async_copy(wq_ref.at[:, sl], wqv.at[n % 2], q_s.at[n % 2])

    def load_o(n):
        sl = pl.ds(pl.multiple_of(n * qw, qw), qw)
        return pltpu.make_async_copy(wo_ref.at[sl], wov.at[n % 2], o_s.at[n % 2])

    def load_kv(g, j):
        sl = pl.ds(pl.multiple_of(g * HEAD, HEAD), HEAD)
        return pltpu.make_async_copy((wk_ref, wv_ref)[j].at[:, sl], (wkv, wvv)[j].at[g % 2], kv_s.at[g % 2, j])

    def load_r():
        return pltpu.make_async_copy(wr_ref, wrv, wr_s.at[0])

    def pass_on(n):
        for link in range(2):
            own(link, n).wait_recv()
            if n < CH // 2:
                relay(link, n).start()
            fwd(link, n).start()

    @pl.when(i == 0)
    def _():
        barrier = pltpu.get_barrier_semaphore()
        for s in range(1, 8):
            pl.semaphore_signal(barrier, inc=1, device_id={'ep': peers[s]}, device_id_type=MESH)
        uu = _rms_rows(h0_ref[...], nm_ref[...])
        u[0] = uu
        pl.semaphore_wait(barrier, 7)
        for n in range(CH):
            for link in range(2):
                own(link, n).start()
        part().start()
        load_r().start()
        load_q(0).start()
        for j in range(2):
            load_kv(0, j).start()
        xs[7, 0:t] = _rms_rows(h0_ref[...], na_ref[...])
        k = ix_ref.shape[1]
        load_r().wait()
        lt = _dot(uu, wrv[...]).T
        it = ix_ref[0]
        ids = lax.broadcasted_iota(jnp.int32, lt.shape, 0)
        sel = [jnp.sum(jnp.where(ids == it[j:j + 1, :], lt, 0.0), axis=0, keepdims=True) for j in range(k)]
        lg = jnp.concatenate(sel, axis=0)
        ex = jnp.exp(lg - jnp.max(lg, axis=0, keepdims=True))
        meta[0, 0:k, :] = it.astype(F32)
        meta[0, k:2 * k, :] = sl_ref[0].astype(F32)
        meta[0, 2 * k:3 * k, :] = ex / jnp.sum(ex, axis=0, keepdims=True)
        acc[...] = h0_ref[...].astype(F32)

    @pl.when(i == 1)
    def _():
        for s in range(1, 8):
            met(s).start()

    @pl.when(i == ATT // 2)
    def _():
        for e in range(RING):
            for j in range(2):
                weights(e, j).start()

    @pl.when(i + 1 < ATT)
    def _():
        load_q(i + 1).start()

    @pl.when(i < ATT)
    def _():
        load_o(i).start()

    @pl.when((i % 2 == 1) & (i + 1 < ATT))
    def _():
        for j in range(2):
            load_kv((i + 1) // 2, j).start()

    for n in range(CH):
        @pl.when(i == PASS[n])
        def _(n=n):
            pass_on(n)

    def rope(v):
        return (v * cos_ref[...] + pltpu.roll(v, HEAD // 2, 1) * sin_ref[...]).astype(BF)

    def project():
        q = _dot(xs[7, 0:t], wqv[i % 2])

        def finish():
            for h in range(hb):
                xs[6 + i % 2, t:2 * t, h * HEAD:(h + 1) * HEAD] = rope(q[:, h * HEAD:(h + 1) * HEAD])
        return finish

    def keys():
        g = (i // 2) % 2
        for j in range(2):
            load_kv(i // 2, j).wait()
        kb[g] = rope(_dot(xs[7, 0:t], wkv[g]))
        vb[g] = _dot(xs[7, 0:t], wvv[g]).astype(BF)

    def attend(between):
        g = ((i - 1) // 2) % 2
        kk, vv = kb[g], vb[g]
        causal = lax.broadcasted_iota(jnp.int32, (t, t), 0) >= lax.broadcasted_iota(jnp.int32, (t, t), 1)
        sc = [lax.dot_general(xs[6 + (i - 1) % 2, t:2 * t, h * HEAD:(h + 1) * HEAD], kk, (((1,), (1,)), ((), ())),
                              preferred_element_type=F32) for h in range(hb)]
        finish = between()
        o = []
        for h in range(hb):
            s = jnp.where(causal, sc[h] * HEAD ** -0.5, -jnp.inf)
            ex = jnp.exp(s - jnp.max(s, axis=1, keepdims=True))
            p = (ex / jnp.sum(ex, axis=1, keepdims=True)).astype(BF)
            o.append(_dot(p, vv).astype(BF))
        finish()
        acc[...] += _dot(jnp.concatenate(o, axis=1), wov[(i - 1) % 2])

    @pl.when((i < ATT) & (i % 2 == 0))
    def _():
        keys()

    @pl.when(i < ATT)
    def _():
        load_q(i).wait()

    @pl.when((i >= 1) & (i <= ATT))
    def _():
        load_o(i - 1).wait()

    @pl.when(i == 0)
    def _():
        project()()

    @pl.when((i >= 1) & (i < ATT))
    def _():
        attend(project)

    @pl.when(i == ATT)
    def _():
        attend(lambda: lambda: None)
        a_ref[...] = acc[...].astype(BF)

    for s in range(8):
        @pl.when(i == D0 + s)
        def _(s=s):
            if s:
                met(s).wait_recv()
            e0 = lax.axis_index('ep') * el
            _places(meta[s], e0.astype(F32), cap, rows, db, gt_ref.at[0])
            if s == 1:
                part().wait_recv()
            if s in (3, 5):
                for n in range(CH):
                    fwd((s - 3) // 2, n).wait_recv()
            if s == 6:
                for n in range(CH // 2):
                    for link in range(2):
                        relay(link, n).wait_recv()
                        fwd3(link, n).start()
            if s == 7:
                for n in range(CH // 2):
                    for link in range(2):
                        fwd3(link, n).wait_recv()
            xs[s] = _dot(db[...], u[s]).astype(BF)

    @pl.when(i == E0)
    def _():
        part().wait_send()
        for link in range(2):
            for n in range(CH):
                own(link, n).wait_send()
                fwd(link, n).wait_send()
                if n < CH // 2:
                    relay(link, n).wait_send()
                    fwd3(link, n).wait_send()
        for q in range(1, 8):
            met(q).wait_send()

        def put(n, p):
            return pltpu.make_async_copy(u.at[n, :, pl.ds(p * d // 2, fe)], hid_ref.at[2 * n + p], hid_s.at[n, p])

        @pl.loop(0, el // 2)
        def _(n):
            for p in range(2):
                e = 2 * n + p
                for j in range(2):
                    weights(e, j).wait()
                x = xs[:, pl.ds(pl.multiple_of(e * cap, cap), cap), :].reshape(8 * cap, d)
                h1 = _dot(x, ring[e % RING, 0])
                h3 = _dot(x, ring[e % RING, 1])
                u[n, :, p * d // 2:p * d // 2 + fe] = (h1 * jax.nn.sigmoid(h1) * h3).astype(BF)

                @pl.when(e < el - RING)
                def _():
                    for j in range(2):
                        weights(e + RING, j).start()

                put(n, p).start()

        @pl.loop(0, el // 2)
        def _(n):
            for p in range(2):
                put(n, p).wait()


def _front(h0, idx, slot, na, nm, cos, sin, wr, wq, wk, wv, wo, ue1, ue3, cap):
    t, d = h0.shape
    el, _, fe = ue1.shape
    rows = el * cap
    qb = wq.shape[1] // ATT
    full = lambda a: pl.BlockSpec(a.shape, lambda i: (0,) * a.ndim, pipeline_mode=pl.Buffered(1))
    one = pl.BlockSpec((t, d), lambda i: (0, 0), pipeline_mode=pl.Buffered(1))

    def src(i):
        s = jnp.clip(i - D0, 0, 7)
        return s // 2 + 4 * (1 - s % 2)

    hbm = pl.BlockSpec(memory_space=pl.ANY)
    dma = pltpu.SemaphoreType.DMA
    return pl.pallas_call(
        lambda *refs: _front_kernel(cap, *refs),
        grid=(E0 + 1,),
        in_specs=[full(h0), full(idx), full(slot), full(na), full(nm), full(cos), full(sin)] + [hbm] * 7,
        out_specs=[hbm,
                   pl.BlockSpec((1, 3 * t, rows), lambda i: (src(i), 0, 0)), one],
        out_shape=[jax.ShapeDtypeStruct((el, 8 * cap, fe), BF), jax.ShapeDtypeStruct((8, 3 * t, rows), BF),
                   jax.ShapeDtypeStruct((t, d), BF)],
        scratch_shapes=[pltpu.VMEM((8, t, d), BF), pltpu.VMEM((8, 3 * idx.shape[1], t), F32),
                        pltpu.VMEM((t, d), F32),
                        pltpu.VMEM((2, t, HEAD), BF), pltpu.VMEM((2, t, HEAD), BF),
                        pltpu.VMEM((8, rows, d), BF), pltpu.VMEM((RING, 2, d, fe), BF),
                        pltpu.VMEM((rows, t), BF), pltpu.VMEM((2, d, qb), BF), pltpu.VMEM((2, d, HEAD), BF),
                        pltpu.VMEM((2, d, HEAD), BF), pltpu.VMEM((2, qb, d), BF), pltpu.VMEM(wr.shape, BF),
                        dma((2, CH)), dma((2, CH)), dma((1,)), dma((1,)), dma((4, CH)), dma((4, CH)),
                        dma((2, CH)), dma((2, CH)), dma((8,)), dma((8,)), dma((RING, 2)), dma((el // 2, 2)),
                        dma((2,)), dma((2, 2)), dma((2,)), dma((1,))],
        compiler_params=pltpu.CompilerParams(dimension_semantics=('arbitrary',), collective_id=0, has_side_effects=True,
                                             vmem_limit_bytes=67043328),
        name='gather_attention_up',
    )(h0, idx, slot, na, nm, cos, sin, wr, wq, wk, wv, wo, ue1, ue3)


NC = 8
FS = 12
LANES = 128
LAG = 2
LATE = 3
POS = ((0, 2, 1, 3), (0, 1, 2, 3))
QE = 2


def _down_kernel(cap, nf_ref, hid_ref, gt_ref, a_ref, ue2_ref, w1_ref, w3_ref, w2_ref, out_ref,
                 hv, gv, ev, w1v, w3v, w2v, hf, yb, mo, mp, r0, r1, r2, acc,
                 h_s, g_s, a_s, e_s, w_s, d_s, d_r, credit, p1_s, p1_r, p2_s, p2_r):
    i = pl.program_id(0)
    peers = _peers()
    el, m, fe = hid_ref.shape
    t, d = a_ref.shape
    nb = d // NC
    fb = w1v.shape[2]
    qe = el // QE

    def rc(src, dst, ss, rs, peer):
        return pltpu.make_async_remote_copy(src_ref=src, dst_ref=dst, send_sem=ss, recv_sem=rs,
                                            device_id={'ep': peer}, device_id_type=MESH)

    def pair(c):
        return rc(mo.at[c % 2], r0.at[c % 2], d_s.at[c % 2], d_r.at[c % 2], peers[1])

    def first(c, b):
        return rc(mp.at[c, b, pl.ds(2, 2)], r1.at[c, b], p1_s.at[c, b], p1_r.at[c, b], peers[2 + 2 * b])

    def second(c, b):
        return rc(mp.at[c, b, 1], r2.at[c, b], p2_s.at[c, b], p2_r.at[c, b], peers[4 - 2 * b])

    def second_step(c):
        for b in range(2):
            first(c, b).wait_recv()
            mp[c, b, pl.ds(0, 2)] = mp[c, b, pl.ds(0, 2)] + r1[c, b]
            second(c, b).start()

    def load_hid(q):
        sl = pl.ds(q * qe, qe)
        return pltpu.make_async_copy(hid_ref.at[sl], hv.at[sl], h_s.at[q])

    def load_gt(q):
        sl = pl.ds(q * 4, 4)
        return pltpu.make_async_copy(gt_ref.at[sl], gv.at[sl], g_s.at[q])

    def load_a():
        return pltpu.make_async_copy(a_ref, out_ref, a_s.at[0])

    def load_down(c, q):
        sl = pl.ds(q * qe, qe)
        return pltpu.make_async_copy(ue2_ref.at[sl, :, pl.ds(pl.multiple_of(c * nb, nb), nb)], ev.at[c % 2, sl],
                                     e_s.at[c % 2, q])

    def load_ffn(n):
        sl = pl.ds(pl.multiple_of(n * fb, fb), fb)
        k = n % 2
        return (pltpu.make_async_copy(w1_ref.at[:, sl], w1v.at[k], w_s.at[k, 0]),
                pltpu.make_async_copy(w3_ref.at[:, sl], w3v.at[k], w_s.at[k, 1]),
                pltpu.make_async_copy(w2_ref.at[sl], w2v.at[k], w_s.at[k, 2]))

    @pl.when(i == 0)
    def _():
        barrier = pltpu.get_barrier_semaphore()
        for s in (1, 2, 4):
            pl.semaphore_signal(barrier, inc=1, device_id={'ep': peers[s]}, device_id_type=MESH)
        for q in range(QE):
            load_hid(q).start()
            load_down(0, q).start()
        for q in range(2):
            load_gt(q).start()
        load_a().start()
        pl.semaphore_wait(barrier, 3)

    def prefetch():
        @pl.when(i + 1 < NC)
        def _():
            for q in range(QE):
                load_down(i + 1, q).start()

        @pl.when(i + 1 < FS)
        def _():
            for cp in load_ffn(i + 1):
                cp.start()

    @pl.when(i > 0)
    def _():
        prefetch()

    @pl.when((i >= LAG) & (i < NC))
    def _():
        second_step(i - LAG)

    for c in range(NC - LAG, NC):
        @pl.when(i == NC + LATE * (c - NC + LAG))
        def _(c=c):
            second_step(c)

    @pl.when(i < NC)
    def _():
        for q in range(QE):
            @pl.when(i == 0)
            def _(q=q):
                load_hid(q).wait()

            load_down(i, q).wait()
            for e in range(q * qe, (q + 1) * qe):
                y = _dot(hv[e], ev[i % 2, e]).astype(BF)
                for s in range(8):
                    yb[s, e * cap:(e + 1) * cap, :] = y[s * cap:(s + 1) * cap]

    @pl.when(i == 0)
    def _():
        load_gt(0).wait()
        for cp in load_ffn(0):
            cp.start()
        prefetch()

    @pl.when((i >= 2) & (i < NC))
    def _():
        pl.semaphore_wait(credit, 1)

    def combine(s):
        v = _dot(gv[s // 2 + 4 * (1 - s % 2)], yb[s])
        v = v[:t] + v[t:2 * t] + v[2 * t:]
        for b in range(2):
            dst = v[:, b * LANES:(b + 1) * LANES]
            if s % 2:
                mo[i % 2, b, POS[b][s // 2]] = dst
            else:
                mp[i, b, POS[b][s // 2]] = dst

    @pl.when(i < NC)
    def _():
        for s in range(1, 8, 2):
            combine(s)
        pair(i).start()

        @pl.when(i == 0)
        def _():
            load_gt(1).wait()

        for s in range(0, 8, 2):
            combine(s)

    @pl.when(i == 0)
    def _():
        load_a().wait()
        acc[...] = out_ref[...].astype(F32)
        out_ref[...] = _rms_rows(out_ref[...], nf_ref[...])

    def exchange():
        pair(i).wait()
        mp[i] = mp[i] + r0[i % 2]

        @pl.when(i < NC - 2)
        def _():
            pl.semaphore_signal(credit, inc=1, device_id={'ep': peers[1]}, device_id_type=MESH)

        for b in range(2):
            first(i, b).start()

    @pl.when(i == 0)
    def _():
        exchange()

    for cp in load_ffn(i):
        cp.wait()
    h1 = _dot(out_ref[...], w1v[i % 2])
    h3 = _dot(out_ref[...], w3v[i % 2])
    hf[...] = (h1 * jax.nn.sigmoid(h1) * h3).astype(BF)

    @pl.when((i > 0) & (i < NC))
    def _():
        exchange()

    acc[...] += _dot(hf[...], w2v[i % 2])

    @pl.when(i == FS - 1)
    def _():
        for c in range(NC):
            for b in range(2):
                second(c, b).wait_recv()
                col = pl.ds((2 * c + b) * LANES, LANES)
                out_ref[:, col] = (acc[:, col] + (mp[c, b, 0] + r2[c, b])).astype(BF)
        for c in range(NC):
            for b in range(2):
                first(c, b).wait_send()
                second(c, b).wait_send()


def _down(hid, gt, a, nf, ue2, w1, w3, w2, cap):
    el, m, fe = hid.shape
    t, d = a.shape
    nb = d // NC
    fb = w1.shape[1] // FS
    hbm = pl.BlockSpec(memory_space=pl.ANY)
    dma = pltpu.SemaphoreType.DMA
    return pl.pallas_call(
        lambda *refs: _down_kernel(cap, *refs),
        grid=(FS,),
        in_specs=[pl.BlockSpec(nf.shape, lambda i: (0,), pipeline_mode=pl.Buffered(1))] + [hbm] * 7,
        out_specs=pl.BlockSpec((t, d), lambda i: (0, 0), pipeline_mode=pl.Buffered(1)),
        out_shape=jax.ShapeDtypeStruct((t, d), BF),
        scratch_shapes=[pltpu.VMEM(hid.shape, BF), pltpu.VMEM(gt.shape, BF),
                        pltpu.VMEM((2, el, fe, nb), BF), pltpu.VMEM((2, d, fb), BF), pltpu.VMEM((2, d, fb), BF),
                        pltpu.VMEM((2, fb, d), BF), pltpu.VMEM((t, fb), BF),
                        pltpu.VMEM((8, el * cap, nb), BF),
                        pltpu.VMEM((2, 2, 4, t, LANES), F32), pltpu.VMEM((NC, 2, 4, t, LANES), F32),
                        pltpu.VMEM((2, 2, 4, t, LANES), F32), pltpu.VMEM((NC, 2, 2, t, LANES), F32),
                        pltpu.VMEM((NC, 2, t, LANES), F32), pltpu.VMEM((t, d), F32),
                        dma((QE,)), dma((2,)), dma((1,)), dma((2, QE)), dma((2, 3)),
                        dma((2,)), dma((2,)), pltpu.SemaphoreType.REGULAR,
                        dma((NC, 2)), dma((NC, 2)), dma((NC, 2)), dma((NC, 2))],
        compiler_params=pltpu.CompilerParams(dimension_semantics=('arbitrary',), collective_id=1, has_side_effects=True,
                                             vmem_limit_bytes=67043328),
        name='expert_down_ffn',
    )(nf, hid, gt, a, ue2, w1, w3, w2)


def solution(mesh):
    G = mesh.shape['ep']

    def local(h0, idx, slot, na, wq, wk, wv, wo, nf, w1, w3, w2, nm, wr, ue1, ue3, ue2):
        b, s, d = h0.shape
        k = idx.shape[-1]
        el = ue1.shape[0]
        cap = 2 * s * k // (el * G)
        cos, sin = _tables(s)
        h = h0.reshape(s, d)
        hid, gt, a = _front(h, jnp.swapaxes(idx, 1, 2), jnp.swapaxes(slot, 1, 2), na, nm, cos, sin, wr, wq, wk, wv,
                               wo, ue1, ue3, cap)
        return _down(hid, gt, a, nf, ue2, w1, w3, w2, cap).reshape(b, s, d)

    rows_spec = P(('dp', 'ep'))
    in_specs = (rows_spec,) * 3 + (P(),) * 11 + (P('ep'),) * 3
    return jax.shard_map(local, mesh=mesh, in_specs=in_specs, out_specs=rows_spec, check_vma=False)
```
